512 devices in a mesh: member: 32 (over y, z_lo, core), tile: 16 (over x, z_hi).
Axes of the slice: x: 4, y: 4, z: 16 (z_hi: 4, z_lo: 4; z = z_hi * 4 + z_lo), core: 2. Of those that a mesh axis runs over, the one named last changes fastest.
Arguments:
- innovations: bfloat16 [32, 4, 256, 1024], P('member', None, None, 'tile'), may hold values from -6 to 6
- obs_column: int32 [4, 1024], P(None, 'tile'), may hold values from 0 to 511
- physics: float32 [4, 256, 256], replicated, as said below
- diffusion: float32 [256], replicated, may hold values from 0.05 to 0.24
- anomalies: bfloat16 [32, 256, 64, 128], P('member', None, 'tile'), may hold values from -6 to 6
- modes: float32 [256, 16], replicated, may hold values from -3 to 3
- bands: int32 [16], replicated, may hold values from 1 to 8
Outputs:
- gradient: float32 [32, 256, 64, 128], P('member', None, 'tile')
The draws below stay inside these ranges and needn't reach their ends.
Inputs may be any that keep to these rules, and one draw needn't show every extreme that they name: `obs_column`: index c = x * 128 + y of an observed column within its tile's 4 by 128 columns; indices may repeat. `physics`: each step's matrix has a dominant diagonal near 0.6.
All inputs are finite; a program needn't handle non-finite values.
Results may differ from the reference program's by a relative error of at most 0.0003.
Values sent between devices are 32-bit elements; how exact they have to be, the bound alone decides.
No kernel may reach another device: no remote copies, remote signals or barrier semaphores. Data moves between devices by JAX's collectives and lax.ppermute only.
A program may use at most 64 MiB of HBM per device.

```python
import jax
import jax.numpy as jnp
from jax import lax

STATE = 256
MODES = 16
STEPS = 4
NY = 128
CX = 4
OBS = 64
MEMBERS = 32
NX = 64
N_TILE = 16


def draw_physics(key, part):
    inner = jax.random.fold_in(key, 17)
    noise = jax.random.normal(inner, (STEPS, STATE, STATE), jnp.float32)
    eye = jnp.eye(STATE, dtype=jnp.float32)[None]
    return 0.6 * eye + 0.4 * noise / jnp.sqrt(jnp.float32(STATE))


def set_ends(drawn, stream_key, least, top_value):
    longest = drawn.shape.index(max(drawn.shape))
    spots = []
    for shift in (0, 1):
        where = [jax.random.randint(jax.random.fold_in(stream_key, axis), (), 0, length) for axis, length in enumerate(drawn.shape)]
        where[longest] = (where[longest] + shift) % drawn.shape[longest]
        spots.append(tuple(where))
    return drawn.at[spots[0]].set(least).at[spots[1]].set(top_value)


def block_scale(rng, dims, cuts, low, top_value):
    factor_of = 1.0
    for position, blocks in cuts:
        heights = jax.random.uniform(jax.random.fold_in(jax.random.fold_in(rng, 6), position), (blocks,), jnp.float32, low / len(cuts), top_value / len(cuts))
        factor_of = factor_of * jnp.repeat(jnp.exp(heights), dims[position] // blocks).reshape((-1,) + (1,) * (len(dims) - 1 - position))
    return factor_of


def centred(key, extent, scale, bound, split=(), held_as=jnp.bfloat16):
    array = jax.random.normal(key, extent, jnp.float32) * scale
    if len(split) > 0:
        array = block_scale(key, extent, split, -0.22, 0.18) * array
    return jnp.clip(array, min=-bound, max=bound).astype(held_as)


def setup_inputs(seed: int = 0) -> dict:
    keys = jax.random.split(jax.random.key(seed), 8)
    return {
        "innovations": centred(keys[0], (MEMBERS, STEPS, STATE, N_TILE * OBS), 1.0, 6.0, ((0, 32), (3, 16))),
        "obs_column": set_ends(jax.random.randint(keys[1], (STEPS, N_TILE * OBS), 0, CX * NY), jax.random.fold_in(keys[1], 1), 0, (CX * NY) - 1).astype(jnp.int32),
        "physics": draw_physics(jax.random.fold_in(keys[7], 71), 0),
        "diffusion": jnp.clip(jax.random.uniform(keys[3], (STATE,), jnp.float32, 0.05, 0.24), 0.05, 0.24),
        "anomalies": centred(keys[4], (MEMBERS, STATE, NX, NY), 1.0, 6.0, ((0, 32), (2, 16))),
        "modes": centred(keys[5], (STATE, MODES), 0.5, 3.0, (), jnp.float32),
        "bands": set_ends(jax.random.randint(keys[6], (MODES,), 1, 9), jax.random.fold_in(keys[6], 1), 1, 8).astype(jnp.int32),
    }


def smooth_modes(coeffs, bands):
    length = coeffs.shape[-1]
    padded = jnp.pad(coeffs, ((0, 0), (0, 0), (8, 8)))
    total = jnp.zeros(coeffs.shape, jnp.float32)
    for offset in range(-8, 9):
        weight = (jnp.abs(jnp.int32(offset)) <= bands).astype(jnp.float32)
        total = total + weight[:, None, None] * padded[:, :, 8 + offset:8 + offset + length]
    return total / (2 * bands + 1).astype(jnp.float32)[:, None, None]


def reference(innovations, obs_column, physics, diffusion, anomalies, modes, bands):
    members = anomalies.shape[0]
    state = anomalies.shape[1]
    spread = anomalies.astype(jnp.float32)
    tiles = obs_column.shape[1] // OBS
    owner = (jnp.arange(tiles * OBS, dtype=jnp.int32) // OBS) * (CX * NY)
    lam = jnp.zeros(anomalies.shape, jnp.float32)
    nu = diffusion[None, :, None, None]
    for step in range(STEPS - 1, -1, -1):
        local = jnp.einsum("sk,msxy->mkxy", modes, spread * lam, precision=lax.Precision.HIGHEST)
        coeffs = jnp.sum(local, axis=0) / jnp.float32(members - 1)
        smooth = smooth_modes(coeffs, bands)
        lifted = jnp.einsum("sk,kxy->sxy", modes, smooth, precision=lax.Precision.HIGHEST)
        moved = jnp.einsum("rs,mrxy->msxy", physics[step], lam, precision=lax.Precision.HIGHEST)
        ypad = jnp.pad(moved, ((0, 0), (0, 0), (0, 0), (1, 1)))
        beside_all = jnp.roll(moved, 1, axis=2) + jnp.roll(moved, -1, axis=2) + ypad[..., 2:] + ypad[..., :-2]
        spread_out = moved + nu * (beside_all - 4.0 * moved)
        flat = owner + obs_column[step].astype(jnp.int32)
        forcing = jnp.zeros((members, state, NX * NY), jnp.float32)
        forcing = forcing.at[:, :, flat].add(innovations[:, step].astype(jnp.float32))
        forcing = forcing.reshape(members, state, NX, NY)
        lam = spread_out + spread * lifted[None] + forcing
    return lam
```

```python
import jax
import jax.numpy as jnp
from jax import lax
from jax.sharding import PartitionSpec as P

STEPS = 4
HI = lax.Precision.HIGHEST


def band_matrix(band, length):
    pos = jnp.arange(length, dtype=jnp.int32)
    near = jnp.abs(pos[:, None] - pos[None, :]) <= band
    return near.astype(jnp.float32)


def summed_smooth(local, near, scale):
    members = lax.axis_size("member")
    modes, width_x, width_y = local.shape
    pieces = local.reshape(members, modes * width_x // members, width_y)
    mine = lax.all_to_all(pieces, "member", 0, 0, tiled=True).sum(axis=0)
    mine = jnp.dot(mine, near, precision=HI) * scale
    copies = jnp.broadcast_to(mine[None], (members, *mine.shape))
    whole = lax.all_to_all(copies, "member", 0, 0, tiled=True)
    return whole.reshape(modes, width_x, width_y)


def edges_from_neighbours(field, axis):
    count = lax.axis_size(axis)
    forward = [(i, (i + 1) % count) for i in range(count)]
    backward = [(target, source) for source, target in forward]
    low = lax.ppermute(field[:, -1:], axis, forward)
    high = lax.ppermute(field[:, :1], axis, backward)
    return low, high


def diffuse(padded, nu):
    center = padded[:, 1:-1]
    ypad = jnp.pad(center, ((0, 0), (0, 0), (1, 1)))
    beside_all = padded[:, 2:] + padded[:, :-2] + ypad[:, :, 2:] + ypad[:, :, :-2]
    return center + nu[:, None, None] * (beside_all - 4.0 * center)


def per_device(innovations, obs_column, physics, diffusion, anomalies, modes, bands):
    members = lax.axis_size("member")
    spread = anomalies[0].astype(jnp.float32)
    state, width_x, width_y = spread.shape
    columns = jnp.arange(width_x * width_y, dtype=jnp.int32)
    rows_each = modes.shape[1] * width_x // members
    mode = lax.axis_index("member") * rows_each // width_x
    band = lax.dynamic_index_in_dim(bands, mode, keepdims=False)
    near = band_matrix(band, width_y)
    scale = 1.0 / ((members - 1) * (2 * band + 1)).astype(jnp.float32)

    def forcing(step):
        onehot = (obs_column[step][:, None] == columns[None, :]).astype(jnp.bfloat16)
        out = jnp.dot(innovations[0, step], onehot, preferred_element_type=jnp.float32)
        return out.reshape(state, width_x, width_y)

    lam = forcing(STEPS - 1)
    for step in range(STEPS - 2, -1, -1):
        local = jnp.einsum("sk,sxy->kxy", modes, spread * lam, precision=HI)
        smooth = summed_smooth(local, near, scale)
        moved = jnp.einsum("rs,rxy->sxy", physics[step], lam, precision=HI)
        low, high = edges_from_neighbours(moved, "tile")
        padded = jnp.concatenate([low, moved, high], axis=1)
        spread_out = diffuse(padded, diffusion)
        lifted = jnp.einsum("sk,kxy->sxy", modes, smooth, precision=HI)
        lam = spread_out + spread * lifted + forcing(step)
    return lam[None]


def solution(mesh):
    in_specs = (
        P("member", None, None, "tile"),
        P(None, "tile"),
        P(),
        P(),
        P("member", None, "tile", None),
        P(),
        P(),
    )
    out_specs = P("member", None, "tile", None)
    return jax.shard_map(
        per_device, mesh=mesh, in_specs=in_specs, out_specs=out_specs, check_vma=False
    )
```

```python
import functools

import jax
import jax.numpy as jnp
from jax import lax
from jax.experimental import pallas as pl
from jax.experimental.pallas import tpu as pltpu
from jax.sharding import PartitionSpec as P

STEPS = 4
REACH = 8
HI = lax.Precision.HIGHEST
VMEM = 24 << 20
PLANES = 4


def dot(a, b, dims=(((1,), (0,)), ((), ()))):
    return lax.dot_general(a, b, dims, precision=HI, preferred_element_type=jnp.float32)


def forcing_of(core, obs_row, values, width_y):
    count = obs_row.shape[1]
    y = lax.broadcasted_iota(jnp.int32, (width_y, count), 0)
    hot = []
    for i in range(2):
        x = jnp.where(core == 0, i, 3 - i)
        hot.append((obs_row == x * width_y + y).astype(jnp.bfloat16))
    hot = jnp.concatenate(hot, axis=0)
    return lax.dot_general(values, hot, (((0,), (1,)), ((), ())), preferred_element_type=jnp.float32)


def forcings(step, core, obs_ref, mine_ref, other_ref, width_y):
    row = obs_ref[step : step + 1, :]
    count = row.shape[1]
    other = other_ref[step * count : (step + 1) * count, :].astype(jnp.bfloat16)
    return (
        forcing_of(core, row, mine_ref[0, step], width_y),
        forcing_of(core, row, other, width_y),
    )


def send_parts(step, lam, spread, physics_ref, modes_ref, far_ref, near_ref, kept_ref, sums_ref, width_y):
    product = spread[0] * lam[0] + spread[1] * lam[1]
    local = dot(modes_ref[...], product)
    for copy in range(PLANES):
        sums_ref[copy] = local
    w = width_y
    for m in range(2):
        moved = dot(physics_ref[step], lam[m], (((0,), (0,)), ((), ())))
        kept_ref[:, 2 * m * w : (2 * m + 2) * w] = moved
        far_ref[:, m * w : (m + 1) * w] = moved[:, :w]
        near_ref[:, m * w : (m + 1) * w] = moved[:, w:]


def prepare_kernel(width_y, core_ref, mine_ref, anomalies_ref, own_a_ref, given_ref):
    low = core_ref[0] == 0
    w = width_y
    rows = [anomalies_ref[0, :, x, :].astype(jnp.float32) for x in range(4)]
    state = rows[0].shape[0]
    for i in range(2):
        own_a_ref[:, i * w : (i + 1) * w] = jnp.where(low, rows[i], rows[3 - i])
        given_ref[:state, i * w : (i + 1) * w] = jnp.where(low, rows[3 - i], rows[i])
    count = mine_ref.shape[2]
    for t in range(STEPS):
        given_ref[state + t * count : state + (t + 1) * count, :] = mine_ref[0, t].astype(jnp.float32)


def first_kernel(step, width_y, core_ref, obs_ref, mine_ref, own_a_ref, given_ref, physics_ref, modes_ref,
                 far_ref, near_ref, kept_ref, sums_ref):
    core = core_ref[0]
    state = own_a_ref.shape[0]
    lam = forcings(step, core, obs_ref, mine_ref, given_ref.at[state:], width_y)
    spread = (own_a_ref[...], given_ref[:state])
    send_parts(step - 1, lam, spread, physics_ref, modes_ref, far_ref, near_ref, kept_ref, sums_ref, width_y)


def smooth_of(total, bands, width_y, members):
    lane = lax.broadcasted_iota(jnp.int32, (total.shape[0], width_y), 1)
    halves = []
    for i in range(2):
        here = total[:, i * width_y : (i + 1) * width_y]
        out = here
        for off in range(1, REACH + 1):
            up = jnp.where(lane >= off, pltpu.roll(here, off, 1), 0.0)
            down = jnp.where(lane < width_y - off, pltpu.roll(here, width_y - off, 1), 0.0)
            out = out + jnp.where(bands >= off, up + down, 0.0)
        halves.append(out)
    whole = jnp.concatenate(halves, axis=1)
    return whole / ((members - 1) * (2 * bands + 1)).astype(jnp.float32)


def beside(row, width_y):
    lane = lax.broadcasted_iota(jnp.int32, row.shape, 1)
    up = jnp.where(lane >= 1, pltpu.roll(row, 1, 1), 0.0)
    down = jnp.where(lane < width_y - 1, pltpu.roll(row, width_y - 1, 1), 0.0)
    return up + down


def next_lam(step, width_y, members, core_ref, obs_ref, mine_ref, own_a_ref, given_ref, modes_ref,
             bands_ref, nu_ref, sums_ref, kept_ref, far_ref, near_ref):
    w = width_y
    total = sums_ref[0] + sums_ref[1] + sums_ref[2] + sums_ref[3]
    smooth = smooth_of(total, bands_ref[...], w, members)
    lifted = dot(modes_ref[...], smooth, (((0,), (0,)), ((), ())))
    nu = nu_ref[...]
    state = own_a_ref.shape[0]
    spread = (own_a_ref[...], given_ref[:state])
    force = forcings(step, core_ref[0], obs_ref, mine_ref, given_ref.at[state:], w)
    lam = []
    for m in range(2):
        far = kept_ref[:, (2 * m) * w : (2 * m + 1) * w]
        near = kept_ref[:, (2 * m + 1) * w : (2 * m + 2) * w]
        out_far = far_ref[:, (1 - m) * w : (2 - m) * w]
        out_near = near_ref[:, (1 - m) * w : (2 - m) * w]
        v_far = far + nu * (out_far + near + beside(far, w) - 4.0 * far)
        v_near = near + nu * (far + out_near + beside(near, w) - 4.0 * near)
        lam.append(jnp.concatenate([v_far, v_near], axis=1) + spread[m] * lifted + force[m])
    return lam, spread


def step_kernel(step, width_y, members, core_ref, obs_ref, mine_ref, own_a_ref, given_ref, physics_ref,
                modes_ref, bands_ref, nu_ref, sums_ref, kept_ref, far_ref, near_ref,
                far_out, near_out, kept_out, sums_out):
    lam, spread = next_lam(step, width_y, members, core_ref, obs_ref, mine_ref, own_a_ref, given_ref,
                           modes_ref, bands_ref, nu_ref, sums_ref, kept_ref, far_ref, near_ref)
    send_parts(step - 1, lam, spread, physics_ref, modes_ref, far_out, near_out, kept_out, sums_out, width_y)


def last_kernel(step, width_y, members, core_ref, obs_ref, mine_ref, own_a_ref, given_ref,
                modes_ref, bands_ref, nu_ref, sums_ref, kept_ref, far_ref, near_ref, own_out, other_out):
    lam, _ = next_lam(step, width_y, members, core_ref, obs_ref, mine_ref, own_a_ref, given_ref,
                      modes_ref, bands_ref, nu_ref, sums_ref, kept_ref, far_ref, near_ref)
    own_out[...] = lam[0]
    other_out[...] = lam[1]


def finish_kernel(width_y, core_ref, own_ref, back_ref, out_ref):
    low = core_ref[0] == 0
    w = width_y
    mine = (own_ref[:, :w], own_ref[:, w:])
    got = (back_ref[:, :w], back_ref[:, w:])
    when_low = (mine[0], mine[1], got[1], got[0])
    when_high = (got[0], got[1], mine[1], mine[0])
    for x in range(4):
        out_ref[0, :, x, :] = jnp.where(low, when_low[x], when_high[x])


def call(kernel, args, outs, flops=400_000_000):
    return pl.pallas_call(
        kernel,
        in_specs=[pl.BlockSpec(memory_space=pltpu.SMEM)] + [pl.BlockSpec(memory_space=pltpu.VMEM)] * (len(args) - 1),
        out_specs=[pl.BlockSpec(memory_space=pltpu.VMEM)] * len(outs),
        out_shape=[jax.ShapeDtypeStruct(o, jnp.float32) for o in outs],
        cost_estimate=pl.CostEstimate(flops=flops, bytes_accessed=2_000_000, transcendentals=0),
        compiler_params=pltpu.CompilerParams(vmem_limit_bytes=VMEM),
    )(*args)


def per_device(innovations, obs_column, physics, diffusion, anomalies, modes, bands):
    members = lax.axis_size("member")
    tiles = lax.axis_size("tile")
    _, state, _, width_y = anomalies.shape
    core = (lax.axis_index("member") & 1).astype(jnp.int32)[None]
    mine = jnp.swapaxes(innovations, 2, 3)
    count = mine.shape[2]
    modes_t = modes.T
    n_modes = modes.shape[1]

    swap = [(i, i ^ 1) for i in range(members)]
    far_pairs = []
    for m in range(members):
        for t in range(tiles):
            target = (t + 1) % tiles if m % 2 else (t - 1) % tiles
            far_pairs.append((m * tiles + t, (m ^ 1) * tiles + target))
    side = 2 * PLANES
    first_groups = [[side * y + j for y in range(PLANES)] for j in range(side)]
    second_groups = [[side * y + 2 * z + c for z in range(PLANES)] for y in range(PLANES) for c in range(2)]

    half = (state, 2 * width_y)
    full = (state, 4 * width_y)
    sums_shape = (PLANES, n_modes, 2 * width_y)
    own_a, given = call(
        functools.partial(prepare_kernel, width_y),
        (core, mine, anomalies),
        [half, (state + STEPS * count, 2 * width_y)],
    )
    given = lax.ppermute(given, "member", swap)
    bands_col = bands[:, None]
    nu_col = diffusion[:, None]

    step = STEPS - 1
    sent = call(
        functools.partial(first_kernel, step, width_y),
        (core, obs_column, mine, own_a, given, physics, modes_t),
        [half, half, full, sums_shape],
    )
    for step in range(STEPS - 2, -1, -1):
        far, near, kept, sums = sent
        sums = lax.all_to_all(sums, "member", 0, 0, tiled=True, axis_index_groups=first_groups)
        far = lax.ppermute(far, ("member", "tile"), far_pairs)
        near = lax.ppermute(near, "member", swap)
        sums = jnp.broadcast_to(sums.sum(axis=0)[None], sums_shape)
        sums = lax.all_to_all(sums, "member", 0, 0, tiled=True, axis_index_groups=second_groups)
        tail = (modes_t, bands_col, nu_col, sums, kept, far, near)
        if step > 0:
            sent = call(
                functools.partial(step_kernel, step, width_y, members),
                (core, obs_column, mine, own_a, given, physics) + tail,
                [half, half, full, sums_shape],
            )
        else:
            own, other = call(
                functools.partial(last_kernel, step, width_y, members),
                (core, obs_column, mine, own_a, given) + tail,
                [half, half],
            )
    back = lax.ppermute(other, "member", swap)
    return call(functools.partial(finish_kernel, width_y), (core, own, back), [(1, *anomalies.shape[1:])])[0]


def solution(mesh):
    in_specs = (
        P("member", None, None, "tile"),
        P(None, "tile"),
        P(),
        P(),
        P("member", None, "tile", None),
        P(),
        P(),
    )
    out_specs = P("member", None, "tile", None)
    return jax.shard_map(
        per_device, mesh=mesh, in_specs=in_specs, out_specs=out_specs, check_vma=False
    )
```

```python
import functools

import jax
import jax.numpy as jnp
from jax import lax
from jax.experimental import pallas as pl
from jax.experimental.pallas import tpu as pltpu
from jax.sharding import PartitionSpec as P

STEPS = 4
REACH = 8
VMEM = 24 << 20
PLANES = 4


MM = (((1,), (0,)), ((), ()))
TM = (((0,), (0,)), ((), ()))


def halves(x):
    high = x.astype(jnp.bfloat16)
    return high, (x - high.astype(jnp.float32)).astype(jnp.bfloat16)


def dot(a, b, dims=MM):
    part = lambda p, q: lax.dot_general(p, q, dims, preferred_element_type=jnp.float32)
    a_high, a_low = halves(a)
    b_high, b_low = halves(b)
    return part(a_high, b_high) + (part(a_high, b_low) + part(a_low, b_high))


def forcing_of(core, obs_row, values, width_y):
    count = obs_row.shape[1]
    y = lax.broadcasted_iota(jnp.int32, (width_y, count), 0)
    hot = []
    for i in range(2):
        x = jnp.where(core == 0, i, 3 - i)
        hot.append((obs_row == x * width_y + y).astype(jnp.bfloat16))
    hot = jnp.concatenate(hot, axis=0)
    return lax.dot_general(values, hot, (((0,), (1,)), ((), ())), preferred_element_type=jnp.float32)


def forcings(step, core, obs_ref, mine_ref, other_ref, width_y):
    row = obs_ref[step : step + 1, :]
    count = row.shape[1]
    other = other_ref[step * count : (step + 1) * count, :].astype(jnp.bfloat16)
    return (
        forcing_of(core, row, mine_ref[0, step], width_y),
        forcing_of(core, row, other, width_y),
    )


def fetch(step, physics_ref, matrix, sem):
    return pltpu.make_async_copy(physics_ref.at[step], matrix, sem)


def send_parts(lam, spread, physics, modes_ref, far_ref, near_ref, sums_ref, width_y):
    product = spread[0] * lam[0] + spread[1] * lam[1]
    local = dot(modes_ref[...], product)
    for copy in range(PLANES):
        sums_ref[copy] = local
    w = width_y
    physics[0].wait()
    matrix = physics[1][...]
    for m in range(2):
        moved = dot(matrix, lam[m], TM)
        far_ref[:, m * w : (m + 1) * w] = moved[:, :w]
        near_ref[:, m * w : (m + 1) * w] = moved[:, w:]


def prepare_kernel(width_y, core_ref, mine_hbm, anomalies_hbm, own_a_ref, given_ref, mine_ref, anomalies_ref, sems):
    copies = (
        pltpu.make_async_copy(anomalies_hbm, anomalies_ref, sems.at[0]),
        pltpu.make_async_copy(mine_hbm, mine_ref, sems.at[1]),
    )
    for copy in copies:
        copy.start()
    low = core_ref[0] == 0
    w = width_y
    copies[0].wait()
    rows = [anomalies_ref[0, :, x, :].astype(jnp.float32) for x in range(4)]
    state = rows[0].shape[0]
    for i in range(2):
        own_a_ref[:, i * w : (i + 1) * w] = jnp.where(low, rows[i], rows[3 - i]).astype(jnp.bfloat16)
        given_ref[:state, i * w : (i + 1) * w] = jnp.where(low, rows[3 - i], rows[i])
    count = mine_ref.shape[2]
    copies[1].wait()
    for t in range(STEPS):
        given_ref[state + t * count : state + (t + 1) * count, :] = mine_ref[0, t].astype(jnp.float32)


def both_spreads(own_a_ref, other_a_ref):
    return own_a_ref[...].astype(jnp.float32), other_a_ref[...].astype(jnp.float32)


def first_kernel(step, width_y, core_ref, obs_ref, mine_ref, own_a_ref, given_ref, physics_ref, modes_ref,
                 far_ref, near_ref, sums_ref, other_a_ref, other_ref, matrix, sem):
    copy = fetch(step - 1, physics_ref, matrix, sem)
    copy.start()
    state = own_a_ref.shape[0]
    other_a_ref[...] = given_ref[:state, :].astype(jnp.bfloat16)
    other_ref[...] = given_ref[state:, :].astype(jnp.bfloat16)
    lam = forcings(step, core_ref[0], obs_ref, mine_ref, other_ref, width_y)
    spread = both_spreads(own_a_ref, other_a_ref)
    send_parts(lam, spread, (copy, matrix), modes_ref, far_ref, near_ref, sums_ref, width_y)


def smooth_of(total, bands, width_y, members):
    lane = lax.broadcasted_iota(jnp.int32, (total.shape[0], width_y), 1)
    halves = []
    for i in range(2):
        here = total[:, i * width_y : (i + 1) * width_y]
        out = here
        for off in range(1, REACH + 1):
            up = jnp.where(lane >= off, pltpu.roll(here, off, 1), 0.0)
            down = jnp.where(lane < width_y - off, pltpu.roll(here, width_y - off, 1), 0.0)
            out = out + jnp.where(bands >= off, up + down, 0.0)
        halves.append(out)
    whole = jnp.concatenate(halves, axis=1)
    return whole / ((members - 1) * (2 * bands + 1)).astype(jnp.float32)


def beside(row, width_y):
    lane = lax.broadcasted_iota(jnp.int32, row.shape, 1)
    up = jnp.where(lane >= 1, pltpu.roll(row, 1, 1), 0.0)
    down = jnp.where(lane < width_y - 1, pltpu.roll(row, width_y - 1, 1), 0.0)
    return up + down


def next_lam(step, width_y, members, core_ref, obs_ref, mine_ref, own_a_ref, other_a_ref, other_ref, modes_ref,
             bands_ref, nu_ref, sums_ref, far_sent, near_sent, far_ref, near_ref):
    w = width_y
    total = sums_ref[0] + sums_ref[1] + sums_ref[2] + sums_ref[3]
    smooth = smooth_of(total, bands_ref[...], w, members)
    lifted = dot(modes_ref[...], smooth, TM)
    nu = nu_ref[...]
    spread = both_spreads(own_a_ref, other_a_ref)
    force = forcings(step, core_ref[0], obs_ref, mine_ref, other_ref, w)
    lam = []
    for m in range(2):
        far = far_sent[:, m * w : (m + 1) * w]
        near = near_sent[:, m * w : (m + 1) * w]
        out_far = far_ref[:, (1 - m) * w : (2 - m) * w]
        out_near = near_ref[:, (1 - m) * w : (2 - m) * w]
        v_far = far + nu * (out_far + near + beside(far, w) - 4.0 * far)
        v_near = near + nu * (far + out_near + beside(near, w) - 4.0 * near)
        lam.append(jnp.concatenate([v_far, v_near], axis=1) + spread[m] * lifted + force[m])
    return lam, spread


def step_kernel(step, width_y, members, core_ref, obs_ref, mine_ref, own_a_ref, other_a_ref, other_ref, physics_ref,
                modes_ref, bands_ref, nu_ref, sums_ref, far_sent, near_sent, far_ref, near_ref,
                far_out, near_out, sums_out, matrix, sem):
    copy = fetch(step - 1, physics_ref, matrix, sem)
    copy.start()
    lam, spread = next_lam(step, width_y, members, core_ref, obs_ref, mine_ref, own_a_ref, other_a_ref, other_ref,
                           modes_ref, bands_ref, nu_ref, sums_ref, far_sent, near_sent, far_ref, near_ref)
    send_parts(lam, spread, (copy, matrix), modes_ref, far_out, near_out, sums_out, width_y)


def last_kernel(step, width_y, members, core_ref, obs_ref, mine_ref, own_a_ref, other_a_ref, other_ref,
                modes_ref, bands_ref, nu_ref, sums_ref, far_sent, near_sent, far_ref, near_ref, own_out, other_out):
    lam, _ = next_lam(step, width_y, members, core_ref, obs_ref, mine_ref, own_a_ref, other_a_ref, other_ref,
                      modes_ref, bands_ref, nu_ref, sums_ref, far_sent, near_sent, far_ref, near_ref)
    own_out[...] = lam[0]
    other_out[...] = lam[1]


def finish_kernel(width_y, core_ref, own_ref, back_ref, out_ref):
    low = core_ref[0] == 0
    w = width_y
    mine = (own_ref[:, :w], own_ref[:, w:])
    got = (back_ref[:, :w], back_ref[:, w:])
    when_low = (mine[0], mine[1], got[1], got[0])
    when_high = (got[0], got[1], mine[1], mine[0])
    for x in range(4):
        out_ref[0, :, x, :] = jnp.where(low, when_low[x], when_high[x])


def call(kernel, name, args, outs, types=(), hbm=(), scratch=(), flops=400_000_000):
    spaces = [pltpu.SMEM] + [pltpu.HBM if i in hbm else pltpu.VMEM for i in range(1, len(args))]
    types = tuple(types) or (jnp.float32,) * len(outs)
    return pl.pallas_call(
        kernel,
        in_specs=[pl.BlockSpec(memory_space=space) for space in spaces],
        out_specs=[pl.BlockSpec(memory_space=pltpu.VMEM)] * len(outs),
        out_shape=[jax.ShapeDtypeStruct(o, t) for o, t in zip(outs, types)],
        scratch_shapes=list(scratch),
        cost_estimate=pl.CostEstimate(flops=flops, bytes_accessed=2_000_000, transcendentals=0),
        compiler_params=pltpu.CompilerParams(vmem_limit_bytes=None if name == "prepare" else VMEM),
    )(*args)


def per_device(innovations, obs_column, physics, diffusion, anomalies, modes, bands):
    members = lax.axis_size("member")
    tiles = lax.axis_size("tile")
    _, state, _, width_y = anomalies.shape
    core = (lax.axis_index("member") & 1).astype(jnp.int32)[None]
    mine = jnp.swapaxes(innovations, 2, 3)
    count = mine.shape[2]
    modes_t = modes.T
    n_modes = modes.shape[1]

    swap = [(i, i ^ 1) for i in range(members)]
    far_pairs = []
    for m in range(members):
        for t in range(tiles):
            target = (t + 1) % tiles if m % 2 else (t - 1) % tiles
            far_pairs.append((m * tiles + t, (m ^ 1) * tiles + target))
    side = 2 * PLANES
    first_groups = [[side * y + j for y in range(PLANES)] for j in range(side)]
    second_groups = [[side * y + 2 * z + c for z in range(PLANES)] for y in range(PLANES) for c in range(2)]

    half = (state, 2 * width_y)
    sums_shape = (PLANES, n_modes, 2 * width_y)
    own_a, given = call(
        functools.partial(prepare_kernel, width_y),
        "prepare",
        (core, mine, anomalies),
        [half, (state + STEPS * count, 2 * width_y)],
        types=(jnp.bfloat16, jnp.float32),
        hbm=(1, 2),
        scratch=(
            pltpu.VMEM(mine.shape, mine.dtype),
            pltpu.VMEM(anomalies.shape, anomalies.dtype),
            pltpu.SemaphoreType.DMA((2,)),
        ),
    )
    matrix = (pltpu.VMEM((state, state), jnp.float32), pltpu.SemaphoreType.DMA)
    given = lax.ppermute(given, "member", swap)
    bands_col = bands[:, None]
    nu_col = diffusion[:, None]

    step = STEPS - 1
    *sent, other_a, other_innov = call(
        functools.partial(first_kernel, step, width_y),
        "first",
        (core, obs_column, mine, own_a, given, physics, modes_t),
        [half, half, sums_shape, half, (STEPS * count, state)],
        types=(jnp.float32,) * 3 + (jnp.bfloat16,) * 2,
        hbm=(5,),
        scratch=matrix,
    )
    known = (core, obs_column, mine, own_a, other_a, other_innov)
    for step in range(STEPS - 2, -1, -1):
        far_sent, near_sent, sums = sent
        sums = lax.all_to_all(sums, "member", 0, 0, tiled=True, axis_index_groups=first_groups)
        far = lax.ppermute(far_sent, ("member", "tile"), far_pairs)
        near = lax.ppermute(near_sent, "member", swap)
        sums = jnp.broadcast_to(sums.sum(axis=0)[None], sums_shape)
        sums = lax.all_to_all(sums, "member", 0, 0, tiled=True, axis_index_groups=second_groups)
        tail = (modes_t, bands_col, nu_col, sums, far_sent, near_sent, far, near)
        if step > 0:
            sent = call(
                functools.partial(step_kernel, step, width_y, members),
                f"step{step}",
                known + (physics,) + tail,
                [half, half, sums_shape],
                hbm=(6,),
                scratch=matrix,
            )
        else:
            own, other = call(
                functools.partial(last_kernel, step, width_y, members),
                "last",
                known + tail,
                [half, half],
            )
    back = lax.ppermute(other, "member", swap)
    return call(functools.partial(finish_kernel, width_y), "finish", (core, own, back), [(1, *anomalies.shape[1:])])[0]


def solution(mesh):
    in_specs = (
        P("member", None, None, "tile"),
        P(None, "tile"),
        P(),
        P(),
        P("member", None, "tile", None),
        P(),
        P(),
    )
    out_specs = P("member", None, "tile", None)
    return jax.shard_map(
        per_device, mesh=mesh, in_specs=in_specs, out_specs=out_specs, check_vma=False
    )
```

```python
import functools

import jax
import jax.numpy as jnp
from jax import lax
from jax.experimental import pallas as pl
from jax.experimental.pallas import tpu as pltpu
from jax.sharding import PartitionSpec as P

STEPS = 4
REACH = 8
VMEM = 24 << 20
PLANES = 4


MM = (((1,), (0,)), ((), ()))
TM = (((0,), (0,)), ((), ()))


def halves(x):
    high = x.astype(jnp.bfloat16)
    return high, (x - high.astype(jnp.float32)).astype(jnp.bfloat16)


def dot(a, b, dims=MM):
    part = lambda p, q: lax.dot_general(p, q, dims, preferred_element_type=jnp.float32)
    a_high, a_low = halves(a)
    b_high, b_low = halves(b)
    return part(a_high, b_high) + (part(a_high, b_low) + part(a_low, b_high))


def hot_rows(core, obs_row, sides, width_y):
    count = obs_row.shape[1]
    y = lax.broadcasted_iota(jnp.int32, (width_y, count), 0)
    hot = []
    for side in sides:
        x = jnp.where(core == 0, side, 3 - side)
        hot.append((obs_row == x * width_y + y).astype(jnp.bfloat16))
    return jnp.concatenate(hot, axis=0) if len(hot) > 1 else hot[0]


def placed(values, hot):
    return lax.dot_general(values, hot, (((0,), (1,)), ((), ())), preferred_element_type=jnp.float32)


def send_parts(lam, spread, physics, modes_ref, far_ref, near_ref, sums_ref, width_y):
    product = spread[0] * lam[0] + spread[1] * lam[1]
    local = dot(modes_ref[...], product)
    for copy in range(PLANES):
        sums_ref[copy] = local
    w = width_y
    matrix = physics[...]
    for m in range(2):
        moved = dot(matrix, lam[m], TM)
        far_ref[:, m * w : (m + 1) * w] = moved[:, :w]
        near_ref[:, m * w : (m + 1) * w] = moved[:, w:]


def prepare_kernel(width_y, core_ref, obs_ref, mine_hbm, anomalies_hbm, modes_ref, late_ref, sums_ref,
                   mine_ref, anomalies_ref, sems):
    copies = (
        pltpu.make_async_copy(mine_hbm.at[0, STEPS - 1], mine_ref, sems.at[0]),
        pltpu.make_async_copy(anomalies_hbm, anomalies_ref, sems.at[1]),
    )
    for copy in copies:
        copy.start()
    w = width_y
    order = (0, 1, 3, 2)
    count = obs_ref.shape[1]
    obs_row = obs_ref[STEPS - 1 : STEPS, :]
    y = lax.broadcasted_iota(jnp.int32, (w, count), 0)
    hot = jnp.concatenate([(obs_row == x * w + y).astype(jnp.bfloat16) for x in order], axis=0)
    copies[0].wait()
    values = mine_ref[...]
    late_ref[...] = values.astype(jnp.float32)
    lam = placed(values, hot)
    copies[1].wait()
    spread = jnp.concatenate([anomalies_ref[0, :, x, :].astype(jnp.float32) for x in order], axis=1)
    local = dot(modes_ref[...], spread * lam)
    for copy in range(PLANES):
        sums_ref[copy] = local


def divide_kernel(width_y, core_ref, mine_ref, anomalies_ref, own_a_ref, rest_ref):
    low = core_ref[0] == 0
    w = width_y
    rows = [anomalies_ref[0, :, x, :].astype(jnp.float32) for x in range(4)]
    state = rows[0].shape[0]
    count = mine_ref.shape[2]
    for i in range(2):
        own_a_ref[:, i * w : (i + 1) * w] = jnp.where(low, rows[i], rows[3 - i]).astype(jnp.bfloat16)
        rest_ref[:state, i * w : (i + 1) * w] = jnp.where(low, rows[3 - i], rows[i])
    for t in range(STEPS - 1):
        rest_ref[state + t * count : state + (t + 1) * count, :] = mine_ref[0, t].astype(jnp.float32)


def pass_on_kernel(core_ref, obs_ref, late_ref, other_ref, far_ref):
    count = late_ref.shape[0]
    far_ref[:count, :] = late_ref[...]
    far_ref[count : 2 * count, :] = other_ref[...]
    far_ref[2 * count :, :] = jnp.zeros((far_ref.shape[0] - 2 * count, far_ref.shape[1]), jnp.float32)
    far_ref[2 * count : 2 * count + 1, :count] = obs_ref[STEPS - 1 : STEPS, :].astype(jnp.float32)


def regroup_kernel(core_ref, sums_ref, out_ref):
    total = sums_ref[0] + sums_ref[1] + sums_ref[2] + sums_ref[3]
    half = total.shape[1] // 2
    for j in range(2 * PLANES):
        out_ref[j] = total[:, (j % 2) * half : (j % 2 + 1) * half]


def both_spreads(own_a_ref, other_a_ref):
    return own_a_ref[...].astype(jnp.float32), other_a_ref[...].astype(jnp.float32)


def smooth_of(total, bands, width_y, members):
    lane = lax.broadcasted_iota(jnp.int32, (total.shape[0], width_y), 1)
    halves = []
    for i in range(2):
        here = total[:, i * width_y : (i + 1) * width_y]
        out = here
        for off in range(1, REACH + 1):
            up = jnp.where(lane >= off, pltpu.roll(here, off, 1), 0.0)
            down = jnp.where(lane < width_y - off, pltpu.roll(here, width_y - off, 1), 0.0)
            out = out + jnp.where(bands >= off, up + down, 0.0)
        halves.append(out)
    whole = jnp.concatenate(halves, axis=1)
    return whole / ((members - 1) * (2 * bands + 1)).astype(jnp.float32)


def beside(row, width_y):
    lane = lax.broadcasted_iota(jnp.int32, row.shape, 1)
    up = jnp.where(lane >= 1, pltpu.roll(row, 1, 1), 0.0)
    down = jnp.where(lane < width_y - 1, pltpu.roll(row, width_y - 1, 1), 0.0)
    return up + down


def advance(moved, spread, force, smooth, modes_ref, nu_ref, width_y):
    lifted = dot(modes_ref[...], smooth, TM)
    nu = nu_ref[...]
    lam = []
    for m in range(2):
        far, near, out_near, out_far = moved[m]
        v_far = far + nu * (out_far + near + beside(far, width_y) - 4.0 * far)
        v_near = near + nu * (far + out_near + beside(near, width_y) - 4.0 * near)
        lam.append(jnp.concatenate([v_far, v_near], axis=1) + spread[m] * lifted + force[m])
    return lam


def forcings(step, core, obs_ref, mine_ref, other, width_y):
    hot = hot_rows(core, obs_ref[step : step + 1, :], (0, 1), width_y)
    return placed(mine_ref[0, step], hot), placed(other, hot)


def next_lam(step, width_y, members, core_ref, obs_ref, mine_ref, own_a_ref, other_a_ref, other_ref, modes_ref,
             bands_ref, nu_ref, sums_ref, far_sent, near_sent, far_ref, near_ref):
    w = width_y
    total = sums_ref[0] + sums_ref[1] + sums_ref[2] + sums_ref[3]
    smooth = smooth_of(total, bands_ref[...], w, members)
    spread = both_spreads(own_a_ref, other_a_ref)
    count = obs_ref.shape[1]
    other = other_ref[step * count : (step + 1) * count, :]
    force = forcings(step, core_ref[0], obs_ref, mine_ref, other, w)
    cut = lambda ref, m: ref[:, m * w : (m + 1) * w]
    moved = [
        (cut(far_sent, m), cut(near_sent, m), cut(near_ref, 1 - m), cut(far_ref, 1 - m)) for m in range(2)
    ]
    return advance(moved, spread, force, smooth, modes_ref, nu_ref, w), spread


def second_kernel(width_y, members, core_ref, obs_ref, mine_ref, own_a_ref, rest_ref, late_ref, beyond_ref, first_matrix, matrix,
                  modes_ref, bands_ref, nu_ref, sums_ref,
                  far_out, near_out, sums_out, other_a_ref, other_ref):
    step = STEPS - 2
    core = core_ref[0]
    w = width_y
    state = own_a_ref.shape[0]
    count = obs_ref.shape[1]
    other_a_ref[...] = rest_ref[:state, :].astype(jnp.bfloat16)
    other_ref[...] = rest_ref[state:, :].astype(jnp.bfloat16)
    spread = both_spreads(own_a_ref, other_a_ref)
    hot = hot_rows(core, obs_ref[STEPS - 1 : STEPS, :], (0, 1, 2), w)
    far_hot = hot_rows(core, beyond_ref[2 * count : 2 * count + 1, :count].astype(jnp.int32), (3,), w)
    inside = (mine_ref[0, STEPS - 1], late_ref[...].astype(jnp.bfloat16))
    beyond = [beyond_ref[(1 - m) * count : (2 - m) * count, :].astype(jnp.bfloat16) for m in range(2)]
    turned = first_matrix[...]
    moved = []
    for m in range(2):
        lam = jnp.concatenate([placed(inside[m], hot), placed(beyond[m], far_hot)], axis=1)
        u = dot(turned, lam, TM)
        moved.append([u[:, i * w : (i + 1) * w] for i in range(4)])
    total = sums_ref[0]
    for j in range(1, 2 * PLANES):
        total = total + sums_ref[j]
    smooth = smooth_of(total, bands_ref[...], w, members)
    force = forcings(step, core, obs_ref, mine_ref, other_ref[step * count : (step + 1) * count, :], w)
    lam = advance(moved, spread, force, smooth, modes_ref, nu_ref, w)
    send_parts(lam, spread, matrix, modes_ref, far_out, near_out, sums_out, w)


def step_kernel(step, width_y, members, core_ref, obs_ref, mine_ref, own_a_ref, other_a_ref, other_ref, matrix,
                modes_ref, bands_ref, nu_ref, sums_ref, far_sent, near_sent, far_ref, near_ref,
                far_out, near_out, sums_out):
    lam, spread = next_lam(step, width_y, members, core_ref, obs_ref, mine_ref, own_a_ref, other_a_ref, other_ref,
                           modes_ref, bands_ref, nu_ref, sums_ref, far_sent, near_sent, far_ref, near_ref)
    send_parts(lam, spread, matrix, modes_ref, far_out, near_out, sums_out, width_y)


def last_kernel(step, width_y, members, core_ref, obs_ref, mine_ref, own_a_ref, other_a_ref, other_ref,
                modes_ref, bands_ref, nu_ref, sums_ref, far_sent, near_sent, far_ref, near_ref, own_out, other_out):
    lam, _ = next_lam(step, width_y, members, core_ref, obs_ref, mine_ref, own_a_ref, other_a_ref, other_ref,
                      modes_ref, bands_ref, nu_ref, sums_ref, far_sent, near_sent, far_ref, near_ref)
    own_out[...] = lam[0]
    other_out[...] = lam[1]


def finish_kernel(width_y, core_ref, own_ref, back_ref, out_ref):
    low = core_ref[0] == 0
    w = width_y
    mine = (own_ref[:, :w], own_ref[:, w:])
    got = (back_ref[:, :w], back_ref[:, w:])
    when_low = (mine[0], mine[1], got[1], got[0])
    when_high = (got[0], got[1], mine[1], mine[0])
    for x in range(4):
        out_ref[0, :, x, :] = jnp.where(low, when_low[x], when_high[x])


def call(kernel, name, args, outs, types=(), hbm=(), scratch=(), flops=400_000_000):
    spaces = [pltpu.SMEM] + [pltpu.HBM if i in hbm else pltpu.VMEM for i in range(1, len(args))]
    types = tuple(types) or (jnp.float32,) * len(outs)
    return pl.pallas_call(
        kernel,
        in_specs=[pl.BlockSpec(memory_space=space) for space in spaces],
        out_specs=[pl.BlockSpec(memory_space=pltpu.VMEM)] * len(outs),
        out_shape=[jax.ShapeDtypeStruct(o, t) for o, t in zip(outs, types)],
        scratch_shapes=list(scratch),
        cost_estimate=pl.CostEstimate(flops=flops, bytes_accessed=2_000_000, transcendentals=0),
        compiler_params=pltpu.CompilerParams(vmem_limit_bytes=None if name == "prepare" else VMEM),
    )(*args)


def per_device(innovations, obs_column, physics, diffusion, anomalies, modes, bands):
    members = lax.axis_size("member")
    tiles = lax.axis_size("tile")
    _, state, _, width_y = anomalies.shape
    core = (lax.axis_index("member") & 1).astype(jnp.int32)[None]
    mine = jnp.swapaxes(innovations, 2, 3)
    count = mine.shape[2]
    modes_t = modes.T
    n_modes = modes.shape[1]

    swap = [(i, i ^ 1) for i in range(members)]
    far_pairs = []
    for m in range(members):
        for t in range(tiles):
            target = (t + 1) % tiles if m % 2 else (t - 1) % tiles
            far_pairs.append((m * tiles + t, (m ^ 1) * tiles + target))
    side = 2 * PLANES
    y_groups = [[side * y + j for y in range(PLANES)] for j in range(side)]
    z_groups = [[side * y + 2 * z + c for z in range(PLANES)] for y in range(PLANES) for c in range(2)]
    chip_groups = [[side * y + j for j in range(side)] for y in range(PLANES)]

    half = (state, 2 * width_y)
    sums_shape = (PLANES, n_modes, 2 * width_y)
    bands_col = bands[:, None]
    nu_col = diffusion[:, None]
    late, sums = call(
        functools.partial(prepare_kernel, width_y),
        "prepare",
        (core, obs_column, mine, anomalies, modes_t),
        [(count, state), (PLANES, n_modes, 4 * width_y)],
        hbm=(2, 3),
        scratch=(
            pltpu.VMEM((count, state), mine.dtype),
            pltpu.VMEM(anomalies.shape, anomalies.dtype),
            pltpu.SemaphoreType.DMA((2,)),
        ),
    )
    sums = lax.all_to_all(sums, "member", 0, 0, tiled=True, axis_index_groups=y_groups)
    other_late = lax.ppermute(late, "member", swap)
    (beyond,) = call(pass_on_kernel, "pass_on", (core, obs_column, late, other_late), [(2 * count + 8, state)])
    beyond = lax.ppermute(beyond, ("member", "tile"), far_pairs)
    (sums,) = call(regroup_kernel, "regroup", (core, sums), [(side, n_modes, 2 * width_y)])
    sums = lax.all_to_all(sums, "member", 0, 0, tiled=True, axis_index_groups=chip_groups)
    mine_late, anomalies_late, _ = lax.optimization_barrier((mine, anomalies, other_late))
    own_a, rest = call(
        functools.partial(divide_kernel, width_y),
        "divide",
        (core, mine_late, anomalies_late),
        [half, (state + (STEPS - 1) * count, 2 * width_y)],
        types=(jnp.bfloat16, jnp.float32),
    )
    rest = lax.ppermute(rest, "member", swap)
    *sent, other_a, other_innov = call(
        functools.partial(second_kernel, width_y, members),
        "second",
        (core, obs_column, mine, own_a, rest, other_late, beyond, physics[STEPS - 2], physics[STEPS - 3], modes_t, bands_col, nu_col, sums),
        [half, half, sums_shape, half, ((STEPS - 1) * count, state)],
        types=(jnp.float32,) * 3 + (jnp.bfloat16,) * 2,
    )
    known = (core, obs_column, mine, own_a, other_a, other_innov)
    for step in range(STEPS - 3, -1, -1):
        far_sent, near_sent, sums = sent
        far = lax.ppermute(far_sent, ("member", "tile"), far_pairs)
        sums = lax.all_to_all(sums, "member", 0, 0, tiled=True, axis_index_groups=y_groups)
        near = lax.ppermute(near_sent, "member", swap)
        sums = jnp.broadcast_to(sums.sum(axis=0)[None], sums_shape)
        sums = lax.all_to_all(sums, "member", 0, 0, tiled=True, axis_index_groups=z_groups)
        tail = (modes_t, bands_col, nu_col, sums, far_sent, near_sent, far, near)
        if step > 0:
            sent = call(
                functools.partial(step_kernel, step, width_y, members),
                f"step{step}",
                known + (physics[step - 1],) + tail,
                [half, half, sums_shape],
            )
        else:
            own, other = call(
                functools.partial(last_kernel, step, width_y, members),
                "last",
                known + tail,
                [half, half],
            )
    back = lax.ppermute(other, "member", swap)
    return call(functools.partial(finish_kernel, width_y), "finish", (core, own, back), [(1, *anomalies.shape[1:])])[0]


def solution(mesh):
    in_specs = (
        P("member", None, None, "tile"),
        P(None, "tile"),
        P(),
        P(),
        P("member", None, "tile", None),
        P(),
        P(),
    )
    out_specs = P("member", None, "tile", None)
    return jax.shard_map(
        per_device, mesh=mesh, in_specs=in_specs, out_specs=out_specs, check_vma=False
    )
```

```python
import functools

import jax
import jax.numpy as jnp
from jax import lax
from jax.experimental import pallas as pl
from jax.experimental.pallas import tpu as pltpu
from jax.sharding import PartitionSpec as P

STEPS = 4
REACH = 8
VMEM = 24 << 20
PLANES = 4


MM = (((1,), (0,)), ((), ()))
TM = (((0,), (0,)), ((), ()))


def halves(x):
    high = x.astype(jnp.bfloat16)
    return high, (x - high.astype(jnp.float32)).astype(jnp.bfloat16)


def product(a, b, dims=MM):
    part = lambda p, q: lax.dot_general(p, q, dims, preferred_element_type=jnp.float32)
    return part(a[0], b[0]) + (part(a[0], b[1]) + part(a[1], b[0]))


def dot(a, b, dims=MM):
    return product(halves(a), halves(b), dims)


def hot_rows(core, obs_row, sides, width_y):
    count = obs_row.shape[1]
    y = lax.broadcasted_iota(jnp.int32, (width_y, count), 0)
    hot = []
    for side in sides:
        x = jnp.where(core == 0, side, 3 - side)
        hot.append((obs_row == x * width_y + y).astype(jnp.bfloat16))
    return jnp.concatenate(hot, axis=0) if len(hot) > 1 else hot[0]


def placed(values, hot):
    return lax.dot_general(values, hot, (((0,), (1,)), ((), ())), preferred_element_type=jnp.float32)


def send_parts(lam, spread, turned, modes_ref, far_ref, near_ref, sums_ref, width_y):
    w = width_y
    for m in range(2):
        moved = product(turned, halves(lam[m]))
        far_ref[:, m * w : (m + 1) * w] = moved[:, :w]
        near_ref[:, m * w : (m + 1) * w] = moved[:, w:]
    local = dot(modes_ref[...], spread[0] * lam[0] + spread[1] * lam[1])
    for copy in range(PLANES):
        sums_ref[copy] = local


def turn_kernel(core_ref, physics_ref, high_ref, low_ref):
    for t in range(STEPS - 1):
        high_ref[t], low_ref[t] = halves(jnp.transpose(physics_ref[t]))


def prepare_kernel(width_y, core_ref, obs_ref, mine_hbm, anomalies_hbm, modes_ref, late_ref, sums_ref,
                   mine_ref, anomalies_ref, sems):
    copies = (
        pltpu.make_async_copy(mine_hbm.at[0, STEPS - 1], mine_ref, sems.at[0]),
        pltpu.make_async_copy(anomalies_hbm, anomalies_ref, sems.at[1]),
    )
    for copy in copies:
        copy.start()
    w = width_y
    order = (0, 1, 3, 2)
    count = obs_ref.shape[1]
    obs_row = obs_ref[STEPS - 1 : STEPS, :]
    y = lax.broadcasted_iota(jnp.int32, (w, count), 0)
    hot = jnp.concatenate([(obs_row == x * w + y).astype(jnp.bfloat16) for x in order], axis=0)
    copies[0].wait()
    values = mine_ref[...]
    late_ref[...] = values.astype(jnp.float32)
    lam = placed(values, hot)
    copies[1].wait()
    spread = jnp.concatenate([anomalies_ref[0, :, x, :].astype(jnp.float32) for x in order], axis=1)
    local = dot(modes_ref[...], spread * lam)
    for copy in range(PLANES):
        sums_ref[copy] = local


def divide_kernel(width_y, core_ref, mine_ref, anomalies_ref, own_a_ref, rest_ref):
    low = core_ref[0] == 0
    w = width_y
    rows = [anomalies_ref[0, :, x, :].astype(jnp.float32) for x in range(4)]
    state = rows[0].shape[0]
    count = mine_ref.shape[2]
    for i in range(2):
        own_a_ref[:, i * w : (i + 1) * w] = jnp.where(low, rows[i], rows[3 - i]).astype(jnp.bfloat16)
        rest_ref[:state, i * w : (i + 1) * w] = jnp.where(low, rows[3 - i], rows[i])
    for t in range(STEPS - 1):
        rest_ref[state + t * count : state + (t + 1) * count, :] = mine_ref[0, t].astype(jnp.float32)


def pass_on_kernel(core_ref, obs_ref, late_ref, other_ref, far_ref):
    count = late_ref.shape[0]
    far_ref[:count, :] = late_ref[...]
    far_ref[count : 2 * count, :] = other_ref[...]
    far_ref[2 * count :, :] = jnp.zeros((far_ref.shape[0] - 2 * count, far_ref.shape[1]), jnp.float32)
    far_ref[2 * count : 2 * count + 1, :count] = obs_ref[STEPS - 1 : STEPS, :].astype(jnp.float32)


def regroup_kernel(core_ref, sums_ref, out_ref):
    total = sums_ref[0] + sums_ref[1] + sums_ref[2] + sums_ref[3]
    half = total.shape[1] // 2
    for j in range(2 * PLANES):
        out_ref[j] = total[:, (j % 2) * half : (j % 2 + 1) * half]


def both_spreads(own_a_ref, other_a_ref):
    return own_a_ref[...].astype(jnp.float32), other_a_ref[...].astype(jnp.float32)


def smooth_of(total, bands, width_y, members):
    lane = lax.broadcasted_iota(jnp.int32, (total.shape[0], width_y), 1)
    halves = []
    for i in range(2):
        here = total[:, i * width_y : (i + 1) * width_y]
        out = here
        for off in range(1, REACH + 1):
            up = jnp.where(lane >= off, pltpu.roll(here, off, 1), 0.0)
            down = jnp.where(lane < width_y - off, pltpu.roll(here, width_y - off, 1), 0.0)
            out = out + jnp.where(bands >= off, up + down, 0.0)
        halves.append(out)
    whole = jnp.concatenate(halves, axis=1)
    return whole / ((members - 1) * (2 * bands + 1)).astype(jnp.float32)


def beside(row, width_y):
    lane = lax.broadcasted_iota(jnp.int32, row.shape, 1)
    up = jnp.where(lane >= 1, pltpu.roll(row, 1, 1), 0.0)
    down = jnp.where(lane < width_y - 1, pltpu.roll(row, width_y - 1, 1), 0.0)
    return up + down


def diffused(far, near, out_near, nu, width_y):
    v_far = far + nu * (near + beside(far, width_y) - 4.0 * far)
    v_near = near + nu * (far + out_near + beside(near, width_y) - 4.0 * near)
    return jnp.concatenate([v_far, v_near], axis=1)


def forcings(step, core, obs_ref, mine_ref, other, width_y):
    hot = hot_rows(core, obs_ref[step : step + 1, :], (0, 1), width_y)
    return placed(mine_ref[0, step], hot), placed(other, hot)


def ahead_kernel(width_y, core_ref, obs_ref, mine_ref, rest_ref, late_ref, beyond_ref, high_ref, low_ref, nu_ref,
                 own_g_ref, other_g_ref, other_a_ref, other_ref):
    step = STEPS - 2
    core = core_ref[0]
    w = width_y
    nu = nu_ref[...]
    state = other_a_ref.shape[0]
    count = obs_ref.shape[1]
    other_a_ref[...] = rest_ref[:state, :].astype(jnp.bfloat16)
    other_ref[...] = rest_ref[state:, :].astype(jnp.bfloat16)
    hot = hot_rows(core, obs_ref[STEPS - 1 : STEPS, :], (0, 1, 2), w)
    far_hot = hot_rows(core, beyond_ref[2 * count : 2 * count + 1, :count].astype(jnp.int32), (3,), w)
    inside = (mine_ref[0, STEPS - 1], late_ref[...].astype(jnp.bfloat16))
    beyond = [beyond_ref[(1 - m) * count : (2 - m) * count, :].astype(jnp.bfloat16) for m in range(2)]
    force = forcings(step, core, obs_ref, mine_ref, other_ref[step * count : (step + 1) * count, :], w)
    for m, out_ref in enumerate((own_g_ref, other_g_ref)):
        lam = jnp.concatenate([placed(inside[m], hot), placed(beyond[m], far_hot)], axis=1)
        u = product((high_ref[step], low_ref[step]), halves(lam))
        far, near, out_near, out_far = [u[:, i * w : (i + 1) * w] for i in range(4)]
        g = diffused(far, near, out_near, nu, w) + force[m]
        out_ref[:, :w] = g[:, :w] + nu * out_far
        out_ref[:, w:] = g[:, w:]


def between_kernel(step, width_y, core_ref, obs_ref, mine_ref, other_ref, nu_ref, far_sent, near_sent, near_ref,
                   own_g_ref, other_g_ref):
    w = width_y
    count = obs_ref.shape[1]
    other = other_ref[step * count : (step + 1) * count, :]
    force = forcings(step, core_ref[0], obs_ref, mine_ref, other, w)
    cut = lambda ref, m: ref[:, m * w : (m + 1) * w]
    for m, out_ref in enumerate((own_g_ref, other_g_ref)):
        g = diffused(cut(far_sent, m), cut(near_sent, m), cut(near_ref, 1 - m), nu_ref[...], w)
        out_ref[...] = g + force[m]


def lifted_of(sums_ref, bands_ref, modes_ref, width_y, members):
    total = sums_ref[0]
    for j in range(1, sums_ref.shape[0]):
        total = total + sums_ref[j]
    return dot(modes_ref[...], smooth_of(total, bands_ref[...], width_y, members), TM)


def second_kernel(width_y, members, core_ref, own_a_ref, other_a_ref, high_ref, low_ref, modes_ref, bands_ref, sums_ref,
                  own_g_ref, other_g_ref, far_out, near_out, sums_out):
    lifted = lifted_of(sums_ref, bands_ref, modes_ref, width_y, members)
    spread = both_spreads(own_a_ref, other_a_ref)
    lam = [g_ref[...] + a * lifted for g_ref, a in zip((own_g_ref, other_g_ref), spread)]
    turned = (high_ref[STEPS - 3], low_ref[STEPS - 3])
    send_parts(lam, spread, turned, modes_ref, far_out, near_out, sums_out, width_y)


def joined(g_ref, far_ref, nu, m, width_y):
    w = width_y
    far = g_ref[:, :w] + nu * far_ref[:, (1 - m) * w : (2 - m) * w]
    return jnp.concatenate([far, g_ref[:, w:]], axis=1)


def step_kernel(step, width_y, members, core_ref, own_a_ref, other_a_ref, high_ref, low_ref, modes_ref, bands_ref,
                nu_ref, sums_ref, own_g_ref, other_g_ref, far_ref, far_out, near_out, sums_out):
    lifted = lifted_of(sums_ref, bands_ref, modes_ref, width_y, members)
    spread = both_spreads(own_a_ref, other_a_ref)
    nu = nu_ref[...]
    g = (joined(own_g_ref, far_ref, nu, 0, width_y), joined(other_g_ref, far_ref, nu, 1, width_y))
    lam = [g[m] + spread[m] * lifted for m in range(2)]
    turned = (high_ref[step - 1], low_ref[step - 1])
    send_parts(lam, spread, turned, modes_ref, far_out, near_out, sums_out, width_y)


def last_kernel(member, width_y, members, core_ref, a_ref, modes_ref, bands_ref, nu_ref, sums_ref, g_ref, far_ref, out_ref):
    lifted = lifted_of(sums_ref, bands_ref, modes_ref, width_y, members)
    out_ref[...] = joined(g_ref, far_ref, nu_ref[...], member, width_y) + a_ref[...].astype(jnp.float32) * lifted


def finish_kernel(width_y, core_ref, own_ref, back_ref, out_ref):
    low = core_ref[0] == 0
    w = width_y
    mine = (own_ref[:, :w], own_ref[:, w:])
    got = (back_ref[:, :w], back_ref[:, w:])
    when_low = (mine[0], mine[1], got[1], got[0])
    when_high = (got[0], got[1], mine[1], mine[0])
    for x in range(4):
        out_ref[0, :, x, :] = jnp.where(low, when_low[x], when_high[x])


def call(kernel, name, args, outs, types=(), hbm=(), scratch=(), flops=400_000_000):
    spaces = [pltpu.SMEM] + [pltpu.HBM if i in hbm else pltpu.VMEM for i in range(1, len(args))]
    types = tuple(types) or (jnp.float32,) * len(outs)
    return pl.pallas_call(
        kernel,
        in_specs=[pl.BlockSpec(memory_space=space) for space in spaces],
        out_specs=[pl.BlockSpec(memory_space=pltpu.VMEM)] * len(outs),
        out_shape=[jax.ShapeDtypeStruct(o, t) for o, t in zip(outs, types)],
        scratch_shapes=list(scratch),
        cost_estimate=pl.CostEstimate(flops=flops, bytes_accessed=2_000_000, transcendentals=0),
        compiler_params=pltpu.CompilerParams(vmem_limit_bytes=None if name == "prepare" else VMEM),
    )(*args)


def per_device(innovations, obs_column, physics, diffusion, anomalies, modes, bands):
    members = lax.axis_size("member")
    tiles = lax.axis_size("tile")
    _, state, _, width_y = anomalies.shape
    core = (lax.axis_index("member") & 1).astype(jnp.int32)[None]
    mine = jnp.swapaxes(innovations, 2, 3)
    count = mine.shape[2]
    modes_t = modes.T
    n_modes = modes.shape[1]

    swap = [(i, i ^ 1) for i in range(members)]
    far_pairs = []
    for m in range(members):
        for t in range(tiles):
            target = (t + 1) % tiles if m % 2 else (t - 1) % tiles
            far_pairs.append((m * tiles + t, (m ^ 1) * tiles + target))
    side = 2 * PLANES
    y_groups = [[side * y + j for y in range(PLANES)] for j in range(side)]
    z_groups = [[side * y + 2 * z + c for z in range(PLANES)] for y in range(PLANES) for c in range(2)]
    chip_groups = [[side * y + j for j in range(side)] for y in range(PLANES)]

    half = (state, 2 * width_y)
    sums_shape = (PLANES, n_modes, 2 * width_y)
    bands_col = bands[:, None]
    nu_col = diffusion[:, None]
    late, sums = call(
        functools.partial(prepare_kernel, width_y),
        "prepare",
        (core, obs_column, mine, anomalies, modes_t),
        [(count, state), (PLANES, n_modes, 4 * width_y)],
        hbm=(2, 3),
        scratch=(
            pltpu.VMEM((count, state), mine.dtype),
            pltpu.VMEM(anomalies.shape, anomalies.dtype),
            pltpu.SemaphoreType.DMA((2,)),
        ),
    )
    sums = lax.all_to_all(sums, "member", 0, 0, tiled=True, axis_index_groups=y_groups)
    other_late = lax.ppermute(late, "member", swap)
    (beyond,) = call(pass_on_kernel, "pass_on", (core, obs_column, late, other_late), [(2 * count + 8, state)])
    beyond = lax.ppermute(beyond, ("member", "tile"), far_pairs)
    (sums,) = call(regroup_kernel, "regroup", (core, sums), [(side, n_modes, 2 * width_y)])
    sums = lax.all_to_all(sums, "member", 0, 0, tiled=True, axis_index_groups=chip_groups)
    mine_late, anomalies_late, _ = lax.optimization_barrier((mine, anomalies, other_late))
    own_a, rest = call(
        functools.partial(divide_kernel, width_y),
        "divide",
        (core, mine_late, anomalies_late),
        [half, (state + (STEPS - 1) * count, 2 * width_y)],
        types=(jnp.bfloat16, jnp.float32),
    )
    rest = lax.ppermute(rest, "member", swap)
    physics_late, _ = lax.optimization_barrier((physics, other_late))
    turned = call(turn_kernel, "turn", (core, physics_late), [(STEPS - 1, state, state)] * 2, types=(jnp.bfloat16,) * 2)
    own_g, other_g, other_a, other_innov = call(
        functools.partial(ahead_kernel, width_y),
        "ahead",
        (core, obs_column, mine, rest, other_late, beyond, *turned, nu_col),
        [half, half, half, ((STEPS - 1) * count, state)],
        types=(jnp.float32,) * 2 + (jnp.bfloat16,) * 2,
    )
    spreads = (own_a, other_a)
    far_sent, near_sent, sums = call(
        functools.partial(second_kernel, width_y, members),
        "second",
        (core, *spreads, *turned, modes_t, bands_col, sums, own_g, other_g),
        [half, half, sums_shape],
    )
    for step in range(STEPS - 3, -1, -1):
        far = lax.ppermute(far_sent, ("member", "tile"), far_pairs)
        sums = lax.all_to_all(sums, "member", 0, 0, tiled=True, axis_index_groups=y_groups)
        near = lax.ppermute(near_sent, "member", swap)
        sums = jnp.broadcast_to(sums.sum(axis=0)[None], sums_shape)
        sums = lax.all_to_all(sums, "member", 0, 0, tiled=True, axis_index_groups=z_groups)
        own_g, other_g = call(
            functools.partial(between_kernel, step, width_y),
            f"between{step}",
            (core, obs_column, mine, other_innov, nu_col, far_sent, near_sent, near),
            [half, half],
        )
        if step > 0:
            far_sent, near_sent, sums = call(
                functools.partial(step_kernel, step, width_y, members),
                f"step{step}",
                (core, *spreads, *turned, modes_t, bands_col, nu_col, sums, own_g, other_g, far),
                [half, half, sums_shape],
            )
    ends = []
    for member, g in ((1, other_g), (0, own_g)):
        (end,) = call(
            functools.partial(last_kernel, member, width_y, members),
            f"last{member}",
            (core, spreads[member], modes_t, bands_col, nu_col, sums, g, far),
            [half],
        )
        ends.append(end)
    other, own = ends
    back = lax.ppermute(other, "member", swap)
    return call(functools.partial(finish_kernel, width_y), "finish", (core, own, back), [(1, *anomalies.shape[1:])])[0]


def solution(mesh):
    in_specs = (
        P("member", None, None, "tile"),
        P(None, "tile"),
        P(),
        P(),
        P("member", None, "tile", None),
        P(),
        P(),
    )
    out_specs = P("member", None, "tile", None)
    return jax.shard_map(
        per_device, mesh=mesh, in_specs=in_specs, out_specs=out_specs, check_vma=False
    )
```

```python
import functools

import jax
import jax.numpy as jnp
from jax import lax
from jax.experimental import pallas as pl
from jax.experimental.pallas import tpu as pltpu
from jax.sharding import PartitionSpec as P

STEPS = 4
REACH = 8
VMEM = 24 << 20
PLANES = 4


MM = (((1,), (0,)), ((), ()))
TM = (((0,), (0,)), ((), ()))


def halves(x):
    high = x.astype(jnp.bfloat16)
    return high, (x - high.astype(jnp.float32)).astype(jnp.bfloat16)


def dot(a, b, dims=MM):
    part = lambda p, q: lax.dot_general(p, q, dims, preferred_element_type=jnp.float32)
    a_high, a_low = halves(a)
    b_high, b_low = halves(b)
    return part(a_high, b_high) + (part(a_high, b_low) + part(a_low, b_high))


def hot_rows(core, obs_row, sides, width_y):
    count = obs_row.shape[1]
    y = lax.broadcasted_iota(jnp.int32, (width_y, count), 0)
    hot = []
    for side in sides:
        x = jnp.where(core == 0, side, 3 - side)
        hot.append((obs_row == x * width_y + y).astype(jnp.bfloat16))
    return jnp.concatenate(hot, axis=0) if len(hot) > 1 else hot[0]


def placed(values, hot):
    return lax.dot_general(values, hot, (((0,), (1,)), ((), ())), preferred_element_type=jnp.float32)


def send_parts(lam, spread, physics, modes_ref, far_ref, near_ref, sums_ref, width_y):
    product = spread[0] * lam[0] + spread[1] * lam[1]
    local = dot(modes_ref[...], product)
    for copy in range(PLANES):
        sums_ref[copy] = local
    w = width_y
    matrix = physics[...]
    for m in range(2):
        moved = dot(matrix, lam[m], TM)
        far_ref[:, m * w : (m + 1) * w] = moved[:, :w]
        near_ref[:, m * w : (m + 1) * w] = moved[:, w:]


def prepare_kernel(width_y, core_ref, obs_ref, mine_hbm, anomalies_hbm, modes_ref, late_ref, sums_ref,
                   mine_ref, anomalies_ref, sems):
    copies = (
        pltpu.make_async_copy(mine_hbm.at[0, STEPS - 1], mine_ref, sems.at[0]),
        pltpu.make_async_copy(anomalies_hbm, anomalies_ref, sems.at[1]),
    )
    for copy in copies:
        copy.start()
    w = width_y
    order = (0, 1, 3, 2)
    count = obs_ref.shape[1]
    obs_row = obs_ref[STEPS - 1 : STEPS, :]
    y = lax.broadcasted_iota(jnp.int32, (w, count), 0)
    hot = jnp.concatenate([(obs_row == x * w + y).astype(jnp.bfloat16) for x in order], axis=0)
    copies[0].wait()
    values = mine_ref[...]
    late_ref[:count, :] = values.astype(jnp.float32)
    late_ref[count:, :] = jnp.zeros((late_ref.shape[0] - count, late_ref.shape[1]), jnp.float32)
    late_ref[count : count + 1, :count] = obs_row.astype(jnp.float32)
    lam = placed(values, hot)
    copies[1].wait()
    spread = jnp.concatenate([anomalies_ref[0, :, x, :].astype(jnp.float32) for x in order], axis=1)
    local = dot(modes_ref[...], spread * lam)
    for copy in range(PLANES):
        sums_ref[copy] = local


def divide_kernel(width_y, core_ref, mine_ref, anomalies_ref, own_a_ref, rest_ref):
    low = core_ref[0] == 0
    w = width_y
    rows = [anomalies_ref[0, :, x, :].astype(jnp.float32) for x in range(4)]
    state = rows[0].shape[0]
    count = mine_ref.shape[2]
    for i in range(2):
        own_a_ref[:, i * w : (i + 1) * w] = jnp.where(low, rows[i], rows[3 - i]).astype(jnp.bfloat16)
        rest_ref[:state, i * w : (i + 1) * w] = jnp.where(low, rows[3 - i], rows[i])
    for t in range(STEPS):
        rest_ref[state + t * count : state + (t + 1) * count, :] = mine_ref[0, t].astype(jnp.float32)


def regroup_kernel(core_ref, sums_ref, out_ref):
    total = sums_ref[0] + sums_ref[1] + sums_ref[2] + sums_ref[3]
    half = total.shape[1] // 2
    for j in range(2 * PLANES):
        out_ref[j] = total[:, (j % 2) * half : (j % 2 + 1) * half]


def both_spreads(own_a_ref, other_a_ref):
    return own_a_ref[...].astype(jnp.float32), other_a_ref[...].astype(jnp.float32)


def smooth_of(total, bands, width_y, members):
    lane = lax.broadcasted_iota(jnp.int32, (total.shape[0], width_y), 1)
    halves = []
    for i in range(2):
        here = total[:, i * width_y : (i + 1) * width_y]
        out = here
        for off in range(1, REACH + 1):
            up = jnp.where(lane >= off, pltpu.roll(here, off, 1), 0.0)
            down = jnp.where(lane < width_y - off, pltpu.roll(here, width_y - off, 1), 0.0)
            out = out + jnp.where(bands >= off, up + down, 0.0)
        halves.append(out)
    whole = jnp.concatenate(halves, axis=1)
    return whole / ((members - 1) * (2 * bands + 1)).astype(jnp.float32)


def beside(row, width_y):
    lane = lax.broadcasted_iota(jnp.int32, row.shape, 1)
    up = jnp.where(lane >= 1, pltpu.roll(row, 1, 1), 0.0)
    down = jnp.where(lane < width_y - 1, pltpu.roll(row, width_y - 1, 1), 0.0)
    return up + down


def advance(moved, spread, force, smooth, modes_ref, nu_ref, width_y):
    lifted = dot(modes_ref[...], smooth, TM)
    nu = nu_ref[...]
    lam = []
    for m in range(2):
        far, near, out_near, out_far = moved[m]
        v_far = far + nu * (out_far + near + beside(far, width_y) - 4.0 * far)
        v_near = near + nu * (far + out_near + beside(near, width_y) - 4.0 * near)
        lam.append(jnp.concatenate([v_far, v_near], axis=1) + spread[m] * lifted + force[m])
    return lam


def forcings(step, core, obs_ref, mine_ref, other, width_y):
    hot = hot_rows(core, obs_ref[step : step + 1, :], (0, 1), width_y)
    return placed(mine_ref[0, step], hot), placed(other, hot)


def next_lam(step, width_y, members, core_ref, obs_ref, mine_ref, own_a_ref, other_a_ref, other_ref, modes_ref,
             bands_ref, nu_ref, sums_ref, far_sent, near_sent, far_ref, near_ref):
    w = width_y
    total = sums_ref[0] + sums_ref[1] + sums_ref[2] + sums_ref[3]
    smooth = smooth_of(total, bands_ref[...], w, members)
    spread = both_spreads(own_a_ref, other_a_ref)
    count = obs_ref.shape[1]
    other = other_ref[step * count : (step + 1) * count, :]
    force = forcings(step, core_ref[0], obs_ref, mine_ref, other, w)
    cut = lambda ref, m: ref[:, m * w : (m + 1) * w]
    moved = [
        (cut(far_sent, m), cut(near_sent, m), cut(near_ref, 1 - m), cut(far_ref, 1 - m)) for m in range(2)
    ]
    return advance(moved, spread, force, smooth, modes_ref, nu_ref, w), spread


def second_kernel(width_y, members, core_ref, obs_ref, mine_ref, own_a_ref, rest_ref, own_beyond_ref, other_beyond_ref, first_matrix, matrix,
                  modes_ref, bands_ref, nu_ref, sums_ref,
                  far_out, near_out, sums_out, other_a_ref, other_ref):
    step = STEPS - 2
    core = core_ref[0]
    w = width_y
    state = own_a_ref.shape[0]
    count = obs_ref.shape[1]
    other_a_ref[...] = rest_ref[:state, :].astype(jnp.bfloat16)
    other = rest_ref[state:, :].astype(jnp.bfloat16)
    other_ref[...] = other[: (STEPS - 1) * count]
    spread = both_spreads(own_a_ref, other_a_ref)
    hot = hot_rows(core, obs_ref[STEPS - 1 : STEPS, :], (0, 1, 2), w)
    far_hot = hot_rows(core, own_beyond_ref[count : count + 1, :count].astype(jnp.int32), (3,), w)
    inside = (mine_ref[0, STEPS - 1], other[(STEPS - 1) * count :])
    beyond = [ref[:count, :].astype(jnp.bfloat16) for ref in (own_beyond_ref, other_beyond_ref)]
    turned = first_matrix[...]
    moved = []
    for m in range(2):
        lam = jnp.concatenate([placed(inside[m], hot), placed(beyond[m], far_hot)], axis=1)
        u = dot(turned, lam, TM)
        moved.append([u[:, i * w : (i + 1) * w] for i in range(4)])
    total = sums_ref[0]
    for j in range(1, 2 * PLANES):
        total = total + sums_ref[j]
    smooth = smooth_of(total, bands_ref[...], w, members)
    force = forcings(step, core, obs_ref, mine_ref, other_ref[step * count : (step + 1) * count, :], w)
    lam = advance(moved, spread, force, smooth, modes_ref, nu_ref, w)
    send_parts(lam, spread, matrix, modes_ref, far_out, near_out, sums_out, w)


def step_kernel(step, width_y, members, core_ref, obs_ref, mine_ref, own_a_ref, other_a_ref, other_ref, matrix,
                modes_ref, bands_ref, nu_ref, sums_ref, far_sent, near_sent, far_ref, near_ref,
                far_out, near_out, sums_out):
    lam, spread = next_lam(step, width_y, members, core_ref, obs_ref, mine_ref, own_a_ref, other_a_ref, other_ref,
                           modes_ref, bands_ref, nu_ref, sums_ref, far_sent, near_sent, far_ref, near_ref)
    send_parts(lam, spread, matrix, modes_ref, far_out, near_out, sums_out, width_y)


def last_kernel(member, step, width_y, members, core_ref, obs_ref, values_ref, a_ref, modes_ref, bands_ref, nu_ref, sums_ref,
                far_sent, near_sent, far_ref, near_ref, out_ref):
    w = width_y
    total = sums_ref[0] + sums_ref[1] + sums_ref[2] + sums_ref[3]
    lifted = dot(modes_ref[...], smooth_of(total, bands_ref[...], w, members), TM)
    count = obs_ref.shape[1]
    values = values_ref[step * count : (step + 1) * count, :] if member else values_ref[0, step]
    force = placed(values, hot_rows(core_ref[0], obs_ref[step : step + 1, :], (0, 1), w))
    nu = nu_ref[...]
    cut = lambda ref, m: ref[:, m * w : (m + 1) * w]
    far, near, out_near, out_far = cut(far_sent, member), cut(near_sent, member), cut(near_ref, 1 - member), cut(far_ref, 1 - member)
    v_far = far + nu * (out_far + near + beside(far, w) - 4.0 * far)
    v_near = near + nu * (far + out_near + beside(near, w) - 4.0 * near)
    out_ref[...] = jnp.concatenate([v_far, v_near], axis=1) + a_ref[...].astype(jnp.float32) * lifted + force


def finish_kernel(width_y, core_ref, own_ref, back_ref, out_ref):
    low = core_ref[0] == 0
    w = width_y
    mine = (own_ref[:, :w], own_ref[:, w:])
    got = (back_ref[:, :w], back_ref[:, w:])
    when_low = (mine[0], mine[1], got[1], got[0])
    when_high = (got[0], got[1], mine[1], mine[0])
    for x in range(4):
        out_ref[0, :, x, :] = jnp.where(low, when_low[x], when_high[x])


def call(kernel, name, args, outs, types=(), hbm=(), scratch=(), flops=400_000_000):
    spaces = [pltpu.SMEM] + [pltpu.HBM if i in hbm else pltpu.VMEM for i in range(1, len(args))]
    types = tuple(types) or (jnp.float32,) * len(outs)
    return pl.pallas_call(
        kernel,
        in_specs=[pl.BlockSpec(memory_space=space) for space in spaces],
        out_specs=[pl.BlockSpec(memory_space=pltpu.VMEM)] * len(outs),
        out_shape=[jax.ShapeDtypeStruct(o, t) for o, t in zip(outs, types)],
        scratch_shapes=list(scratch),
        cost_estimate=pl.CostEstimate(flops=flops, bytes_accessed=2_000_000, transcendentals=0),
        compiler_params=pltpu.CompilerParams(vmem_limit_bytes=None if name == "prepare" else VMEM),
    )(*args)


def per_device(innovations, obs_column, physics, diffusion, anomalies, modes, bands):
    members = lax.axis_size("member")
    tiles = lax.axis_size("tile")
    _, state, _, width_y = anomalies.shape
    core = (lax.axis_index("member") & 1).astype(jnp.int32)[None]
    mine = jnp.swapaxes(innovations, 2, 3)
    count = mine.shape[2]
    modes_t = modes.T
    n_modes = modes.shape[1]

    swap = [(i, i ^ 1) for i in range(members)]
    far_pairs = []
    along_pairs = []
    for m in range(members):
        for t in range(tiles):
            after, before = (t + 1) % tiles, (t - 1) % tiles
            far_pairs.append((m * tiles + t, (m ^ 1) * tiles + (after if m % 2 else before)))
            along_pairs.append((m * tiles + t, m * tiles + (before if m % 2 else after)))
    side = 2 * PLANES
    y_groups = [[side * y + j for y in range(PLANES)] for j in range(side)]
    z_groups = [[side * y + 2 * z + c for z in range(PLANES)] for y in range(PLANES) for c in range(2)]
    chip_groups = [[side * y + j for j in range(side)] for y in range(PLANES)]

    half = (state, 2 * width_y)
    sums_shape = (PLANES, n_modes, 2 * width_y)
    bands_col = bands[:, None]
    nu_col = diffusion[:, None]
    late, sums = call(
        functools.partial(prepare_kernel, width_y),
        "prepare",
        (core, obs_column, mine, anomalies, modes_t),
        [(count + 8, state), (PLANES, n_modes, 4 * width_y)],
        hbm=(2, 3),
        scratch=(
            pltpu.VMEM((count, state), mine.dtype),
            pltpu.VMEM(anomalies.shape, anomalies.dtype),
            pltpu.SemaphoreType.DMA((2,)),
        ),
    )
    sums = lax.all_to_all(sums, "member", 0, 0, tiled=True, axis_index_groups=y_groups)
    own_beyond = lax.ppermute(late, ("member", "tile"), along_pairs)
    other_beyond = lax.ppermute(late, ("member", "tile"), far_pairs)
    (sums,) = call(regroup_kernel, "regroup", (core, sums), [(side, n_modes, 2 * width_y)])
    sums = lax.all_to_all(sums, "member", 0, 0, tiled=True, axis_index_groups=chip_groups)
    mine_late, anomalies_late, _ = lax.optimization_barrier((mine, anomalies, late))
    own_a, rest = call(
        functools.partial(divide_kernel, width_y),
        "divide",
        (core, mine_late, anomalies_late),
        [half, (state + STEPS * count, 2 * width_y)],
        types=(jnp.bfloat16, jnp.float32),
    )
    rest = lax.ppermute(rest, "member", swap)
    *sent, other_a, other_innov = call(
        functools.partial(second_kernel, width_y, members),
        "second",
        (core, obs_column, mine, own_a, rest, own_beyond, other_beyond, physics[STEPS - 2], physics[STEPS - 3], modes_t, bands_col, nu_col, sums),
        [half, half, sums_shape, half, ((STEPS - 1) * count, state)],
        types=(jnp.float32,) * 3 + (jnp.bfloat16,) * 2,
    )
    known = (core, obs_column, mine, own_a, other_a, other_innov)
    for step in range(STEPS - 3, -1, -1):
        far_sent, near_sent, sums = sent
        far = lax.ppermute(far_sent, ("member", "tile"), far_pairs)
        sums = lax.all_to_all(sums, "member", 0, 0, tiled=True, axis_index_groups=y_groups)
        near = lax.ppermute(near_sent, "member", swap)
        sums = jnp.broadcast_to(sums.sum(axis=0)[None], sums_shape)
        sums = lax.all_to_all(sums, "member", 0, 0, tiled=True, axis_index_groups=z_groups)
        tail = (modes_t, bands_col, nu_col, sums, far_sent, near_sent, far, near)
        if step > 0:
            sent = call(
                functools.partial(step_kernel, step, width_y, members),
                f"step{step}",
                known + (physics[step - 1],) + tail,
                [half, half, sums_shape],
            )
    ends = []
    for member, values, a in ((1, other_innov, other_a), (0, mine, own_a)):
        (end,) = call(
            functools.partial(last_kernel, member, 0, width_y, members),
            f"last{member}",
            (core, obs_column, values, a) + tail,
            [half],
        )
        ends.append(end)
    other, own = ends
    back = lax.ppermute(other, "member", swap)
    return call(functools.partial(finish_kernel, width_y), "finish", (core, own, back), [(1, *anomalies.shape[1:])])[0]


def solution(mesh):
    in_specs = (
        P("member", None, None, "tile"),
        P(None, "tile"),
        P(),
        P(),
        P("member", None, "tile", None),
        P(),
        P(),
    )
    out_specs = P("member", None, "tile", None)
    return jax.shard_map(
        per_device, mesh=mesh, in_specs=in_specs, out_specs=out_specs, check_vma=False
    )
```

```python
import functools

import jax
import jax.numpy as jnp
from jax import lax
from jax.experimental import pallas as pl
from jax.experimental.pallas import tpu as pltpu
from jax.sharding import PartitionSpec as P

STEPS = 4
REACH = 8
VMEM = 24 << 20
PLANES = 4


MM = (((1,), (0,)), ((), ()))
TM = (((0,), (0,)), ((), ()))


def halves(x):
    high = x.astype(jnp.bfloat16)
    return high, (x - high.astype(jnp.float32)).astype(jnp.bfloat16)


def dot(a, b, dims=MM):
    part = lambda p, q: lax.dot_general(p, q, dims, preferred_element_type=jnp.float32)
    a_high, a_low = halves(a)
    b_high, b_low = halves(b)
    return part(a_high, b_high) + (part(a_high, b_low) + part(a_low, b_high))


def hot_rows(core, obs_row, sides, width_y):
    count = obs_row.shape[1]
    y = lax.broadcasted_iota(jnp.int32, (width_y, count), 0)
    hot = []
    for side in sides:
        x = jnp.where(core == 0, side, 3 - side)
        hot.append((obs_row == x * width_y + y).astype(jnp.bfloat16))
    return jnp.concatenate(hot, axis=0) if len(hot) > 1 else hot[0]


def placed(values, hot):
    return lax.dot_general(values, hot, (((0,), (1,)), ((), ())), preferred_element_type=jnp.float32)


def send_parts(lam, spread, physics, modes_ref, far_ref, near_ref, sums_ref, width_y):
    product = spread[0] * lam[0] + spread[1] * lam[1]
    local = dot(modes_ref[...], product)
    for copy in range(PLANES):
        sums_ref[copy] = local
    w = width_y
    matrix = physics[...]
    for m in range(2):
        moved = dot(matrix, lam[m], TM)
        far_ref[:, m * w : (m + 1) * w] = moved[:, :w]
        near_ref[:, m * w : (m + 1) * w] = moved[:, w:]


def prepare_kernel(width_y, core_ref, obs_ref, mine_hbm, anomalies_hbm, modes_ref, late_ref, sums_ref,
                   mine_ref, anomalies_ref, sems):
    copies = (
        pltpu.make_async_copy(mine_hbm.at[0, STEPS - 1], mine_ref, sems.at[0]),
        pltpu.make_async_copy(anomalies_hbm, anomalies_ref, sems.at[1]),
    )
    for copy in copies:
        copy.start()
    w = width_y
    order = (0, 1, 3, 2)
    count = obs_ref.shape[1]
    obs_row = obs_ref[STEPS - 1 : STEPS, :]
    y = lax.broadcasted_iota(jnp.int32, (w, count), 0)
    hot = jnp.concatenate([(obs_row == x * w + y).astype(jnp.bfloat16) for x in order], axis=0)
    copies[0].wait()
    values = mine_ref[...]
    late_ref[:count, :] = values.astype(jnp.float32)
    late_ref[count:, :] = jnp.zeros((late_ref.shape[0] - count, late_ref.shape[1]), jnp.float32)
    late_ref[count : count + 1, :count] = obs_row.astype(jnp.float32)
    lam = placed(values, hot)
    copies[1].wait()
    spread = jnp.concatenate([anomalies_ref[0, :, x, :].astype(jnp.float32) for x in order], axis=1)
    local = dot(modes_ref[...], spread * lam)
    for copy in range(PLANES):
        sums_ref[copy] = local


def column(row):
    n = row.shape[1]
    same = lax.broadcasted_iota(jnp.int32, (n, n), 0) == lax.broadcasted_iota(jnp.int32, (n, n), 1)
    return jnp.sum(jnp.where(same, row, 0.0), axis=1, keepdims=True)


def divide_kernel(width_y, core_ref, mine_ref, anomalies_ref, bands_ref, nu_ref, own_a_ref, rest_ref, bands_col_ref, nu_col_ref):
    bands_col_ref[...] = column(bands_ref[...].astype(jnp.float32)).astype(jnp.int32)
    nu_col_ref[...] = column(nu_ref[...])
    low = core_ref[0] == 0
    w = width_y
    rows = [anomalies_ref[0, :, x, :].astype(jnp.float32) for x in range(4)]
    state = rows[0].shape[0]
    count = mine_ref.shape[2]
    for i in range(2):
        own_a_ref[:, i * w : (i + 1) * w] = jnp.where(low, rows[i], rows[3 - i]).astype(jnp.bfloat16)
        rest_ref[:state, i * w : (i + 1) * w] = jnp.where(low, rows[3 - i], rows[i])
    for t in range(STEPS):
        rest_ref[state + t * count : state + (t + 1) * count, :] = mine_ref[0, t].astype(jnp.float32)


def regroup_kernel(core_ref, sums_ref, out_ref):
    total = sums_ref[0] + sums_ref[1] + sums_ref[2] + sums_ref[3]
    half = total.shape[1] // 2
    for j in range(2 * PLANES):
        out_ref[j] = total[:, (j % 2) * half : (j % 2 + 1) * half]


def both_spreads(own_a_ref, other_a_ref):
    return own_a_ref[...].astype(jnp.float32), other_a_ref[...].astype(jnp.float32)


def smooth_of(total, bands, width_y, members):
    lane = lax.broadcasted_iota(jnp.int32, (total.shape[0], width_y), 1)
    halves = []
    for i in range(2):
        here = total[:, i * width_y : (i + 1) * width_y]
        out = here
        for off in range(1, REACH + 1):
            up = jnp.where(lane >= off, pltpu.roll(here, off, 1), 0.0)
            down = jnp.where(lane < width_y - off, pltpu.roll(here, width_y - off, 1), 0.0)
            out = out + jnp.where(bands >= off, up + down, 0.0)
        halves.append(out)
    whole = jnp.concatenate(halves, axis=1)
    return whole / ((members - 1) * (2 * bands + 1)).astype(jnp.float32)


def beside(row, width_y):
    lane = lax.broadcasted_iota(jnp.int32, row.shape, 1)
    up = jnp.where(lane >= 1, pltpu.roll(row, 1, 1), 0.0)
    down = jnp.where(lane < width_y - 1, pltpu.roll(row, width_y - 1, 1), 0.0)
    return up + down


def advance(moved, spread, force, smooth, modes_ref, nu_ref, width_y):
    lifted = dot(modes_ref[...], smooth, TM)
    nu = nu_ref[...]
    lam = []
    for m in range(2):
        far, near, out_near, out_far = moved[m]
        v_far = far + nu * (out_far + near + beside(far, width_y) - 4.0 * far)
        v_near = near + nu * (far + out_near + beside(near, width_y) - 4.0 * near)
        lam.append(jnp.concatenate([v_far, v_near], axis=1) + spread[m] * lifted + force[m])
    return lam


def forcings(step, core, obs_ref, mine_ref, other, width_y):
    hot = hot_rows(core, obs_ref[step : step + 1, :], (0, 1), width_y)
    return placed(mine_ref[0, step], hot), placed(other, hot)


def next_lam(step, width_y, members, core_ref, obs_ref, mine_ref, own_a_ref, other_a_ref, other_ref, modes_ref,
             bands_ref, nu_ref, sums_ref, far_sent, near_sent, far_ref, near_ref):
    w = width_y
    total = sums_ref[0] + sums_ref[1] + sums_ref[2] + sums_ref[3]
    smooth = smooth_of(total, bands_ref[...], w, members)
    spread = both_spreads(own_a_ref, other_a_ref)
    count = obs_ref.shape[1]
    other = other_ref[step * count : (step + 1) * count, :]
    force = forcings(step, core_ref[0], obs_ref, mine_ref, other, w)
    cut = lambda ref, m: ref[:, m * w : (m + 1) * w]
    moved = [
        (cut(far_sent, m), cut(near_sent, m), cut(near_ref, 1 - m), cut(far_ref, 1 - m)) for m in range(2)
    ]
    return advance(moved, spread, force, smooth, modes_ref, nu_ref, w), spread


def second_kernel(width_y, members, core_ref, obs_ref, mine_ref, own_a_ref, rest_ref, own_beyond_ref, other_beyond_ref, physics_ref,
                  modes_ref, bands_ref, nu_ref, sums_ref,
                  far_out, near_out, sums_out, other_a_ref, other_ref, first_matrix, matrix, sems):
    step = STEPS - 2
    copies = [pltpu.make_async_copy(physics_ref.at[step - i], (first_matrix, matrix)[i], sems.at[i]) for i in range(2)]
    for copy in copies:
        copy.start()
    core = core_ref[0]
    w = width_y
    state = own_a_ref.shape[0]
    count = obs_ref.shape[1]
    other_a_ref[...] = rest_ref[:state, :].astype(jnp.bfloat16)
    other = rest_ref[state:, :].astype(jnp.bfloat16)
    other_ref[...] = other[: (STEPS - 1) * count]
    spread = both_spreads(own_a_ref, other_a_ref)
    hot = hot_rows(core, obs_ref[STEPS - 1 : STEPS, :], (0, 1, 2), w)
    far_hot = hot_rows(core, own_beyond_ref[count : count + 1, :count].astype(jnp.int32), (3,), w)
    inside = (mine_ref[0, STEPS - 1], other[(STEPS - 1) * count :])
    beyond = [ref[:count, :].astype(jnp.bfloat16) for ref in (own_beyond_ref, other_beyond_ref)]
    copies[0].wait()
    turned = first_matrix[...]
    moved = []
    for m in range(2):
        lam = jnp.concatenate([placed(inside[m], hot), placed(beyond[m], far_hot)], axis=1)
        u = dot(turned, lam, TM)
        moved.append([u[:, i * w : (i + 1) * w] for i in range(4)])
    total = sums_ref[0]
    for j in range(1, 2 * PLANES):
        total = total + sums_ref[j]
    smooth = smooth_of(total, bands_ref[...], w, members)
    force = forcings(step, core, obs_ref, mine_ref, other_ref[step * count : (step + 1) * count, :], w)
    lam = advance(moved, spread, force, smooth, modes_ref, nu_ref, w)
    copies[1].wait()
    send_parts(lam, spread, matrix, modes_ref, far_out, near_out, sums_out, w)


def step_kernel(step, width_y, members, core_ref, obs_ref, mine_ref, own_a_ref, other_a_ref, other_ref, physics_ref,
                modes_ref, bands_ref, nu_ref, sums_ref, far_sent, near_sent, far_ref, near_ref,
                far_out, near_out, sums_out, matrix, sem):
    copy = pltpu.make_async_copy(physics_ref.at[step - 1], matrix, sem)
    copy.start()
    lam, spread = next_lam(step, width_y, members, core_ref, obs_ref, mine_ref, own_a_ref, other_a_ref, other_ref,
                           modes_ref, bands_ref, nu_ref, sums_ref, far_sent, near_sent, far_ref, near_ref)
    copy.wait()
    send_parts(lam, spread, matrix, modes_ref, far_out, near_out, sums_out, width_y)


def last_kernel(member, step, width_y, members, core_ref, obs_ref, values_ref, a_ref, modes_ref, bands_ref, nu_ref, sums_ref,
                far_sent, near_sent, far_ref, near_ref, out_ref):
    w = width_y
    total = sums_ref[0] + sums_ref[1] + sums_ref[2] + sums_ref[3]
    lifted = dot(modes_ref[...], smooth_of(total, bands_ref[...], w, members), TM)
    count = obs_ref.shape[1]
    values = values_ref[step * count : (step + 1) * count, :] if member else values_ref[0, step]
    force = placed(values, hot_rows(core_ref[0], obs_ref[step : step + 1, :], (0, 1), w))
    nu = nu_ref[...]
    cut = lambda ref, m: ref[:, m * w : (m + 1) * w]
    far, near, out_near, out_far = cut(far_sent, member), cut(near_sent, member), cut(near_ref, 1 - member), cut(far_ref, 1 - member)
    v_far = far + nu * (out_far + near + beside(far, w) - 4.0 * far)
    v_near = near + nu * (far + out_near + beside(near, w) - 4.0 * near)
    out_ref[...] = jnp.concatenate([v_far, v_near], axis=1) + a_ref[...].astype(jnp.float32) * lifted + force


def finish_kernel(width_y, core_ref, own_ref, back_ref, out_ref):
    low = core_ref[0] == 0
    w = width_y
    mine = (own_ref[:, :w], own_ref[:, w:])
    got = (back_ref[:, :w], back_ref[:, w:])
    when_low = (mine[0], mine[1], got[1], got[0])
    when_high = (got[0], got[1], mine[1], mine[0])
    for x in range(4):
        out_ref[0, :, x, :] = jnp.where(low, when_low[x], when_high[x])


def call(kernel, name, args, outs, types=(), hbm=(), scratch=(), flops=400_000_000):
    spaces = [pltpu.SMEM] + [pltpu.HBM if i in hbm else pltpu.VMEM for i in range(1, len(args))]
    types = tuple(types) or (jnp.float32,) * len(outs)
    return pl.pallas_call(
        kernel,
        in_specs=[pl.BlockSpec(memory_space=space) for space in spaces],
        out_specs=[pl.BlockSpec(memory_space=pltpu.VMEM)] * len(outs),
        out_shape=[jax.ShapeDtypeStruct(o, t) for o, t in zip(outs, types)],
        scratch_shapes=list(scratch),
        cost_estimate=pl.CostEstimate(flops=flops, bytes_accessed=2_000_000, transcendentals=0),
        compiler_params=pltpu.CompilerParams(vmem_limit_bytes=None if name == "prepare" else VMEM),
    )(*args)


def per_device(innovations, obs_column, physics, diffusion, anomalies, modes, bands):
    members = lax.axis_size("member")
    tiles = lax.axis_size("tile")
    _, state, _, width_y = anomalies.shape
    core = (lax.axis_index("member") & 1).astype(jnp.int32)[None]
    mine = jnp.swapaxes(innovations, 2, 3)
    count = mine.shape[2]
    modes_t = modes.T
    n_modes = modes.shape[1]

    swap = [(i, i ^ 1) for i in range(members)]
    far_pairs = []
    along_pairs = []
    for m in range(members):
        for t in range(tiles):
            after, before = (t + 1) % tiles, (t - 1) % tiles
            far_pairs.append((m * tiles + t, (m ^ 1) * tiles + (after if m % 2 else before)))
            along_pairs.append((m * tiles + t, m * tiles + (before if m % 2 else after)))
    side = 2 * PLANES
    y_groups = [[side * y + j for y in range(PLANES)] for j in range(side)]
    z_groups = [[side * y + 2 * z + c for z in range(PLANES)] for y in range(PLANES) for c in range(2)]
    chip_groups = [[side * y + j for j in range(side)] for y in range(PLANES)]

    half = (state, 2 * width_y)
    matrix = pltpu.VMEM((state, state), jnp.float32)
    sums_shape = (PLANES, n_modes, 2 * width_y)
    late, sums = call(
        functools.partial(prepare_kernel, width_y),
        "prepare",
        (core, obs_column, mine, anomalies, modes_t),
        [(count + 8, state), (PLANES, n_modes, 4 * width_y)],
        hbm=(2, 3),
        scratch=(
            pltpu.VMEM((count, state), mine.dtype),
            pltpu.VMEM(anomalies.shape, anomalies.dtype),
            pltpu.SemaphoreType.DMA((2,)),
        ),
    )
    sums = lax.all_to_all(sums, "member", 0, 0, tiled=True, axis_index_groups=y_groups)
    own_beyond = lax.ppermute(late, ("member", "tile"), along_pairs)
    other_beyond = lax.ppermute(late, ("member", "tile"), far_pairs)
    (sums,) = call(regroup_kernel, "regroup", (core, sums), [(side, n_modes, 2 * width_y)])
    sums = lax.all_to_all(sums, "member", 0, 0, tiled=True, axis_index_groups=chip_groups)
    mine_late, anomalies_late, _ = lax.optimization_barrier((mine, anomalies, late))
    own_a, rest, bands_col, nu_col = call(
        functools.partial(divide_kernel, width_y),
        "divide",
        (core, mine_late, anomalies_late, bands[None], diffusion[None]),
        [half, (state + STEPS * count, 2 * width_y), (n_modes, 1), (state, 1)],
        types=(jnp.bfloat16, jnp.float32, jnp.int32, jnp.float32),
    )
    rest = lax.ppermute(rest, "member", swap)
    *sent, other_a, other_innov = call(
        functools.partial(second_kernel, width_y, members),
        "second",
        (core, obs_column, mine, own_a, rest, own_beyond, other_beyond, physics, modes_t, bands_col, nu_col, sums),
        [half, half, sums_shape, half, ((STEPS - 1) * count, state)],
        types=(jnp.float32,) * 3 + (jnp.bfloat16,) * 2,
        hbm=(7,),
        scratch=(matrix, matrix, pltpu.SemaphoreType.DMA((2,))),
    )
    known = (core, obs_column, mine, own_a, other_a, other_innov)
    for step in range(STEPS - 3, -1, -1):
        far_sent, near_sent, sums = sent
        far = lax.ppermute(far_sent, ("member", "tile"), far_pairs)
        sums = lax.all_to_all(sums, "member", 0, 0, tiled=True, axis_index_groups=y_groups)
        near = lax.ppermute(near_sent, "member", swap)
        sums = jnp.broadcast_to(sums.sum(axis=0)[None], sums_shape)
        sums = lax.all_to_all(sums, "member", 0, 0, tiled=True, axis_index_groups=z_groups)
        tail = (modes_t, bands_col, nu_col, sums, far_sent, near_sent, far, near)
        if step > 0:
            sent = call(
                functools.partial(step_kernel, step, width_y, members),
                f"step{step}",
                known + (physics,) + tail,
                [half, half, sums_shape],
                hbm=(6,),
                scratch=(matrix, pltpu.SemaphoreType.DMA),
            )
    ends = []
    for member, values, a in ((1, other_innov, other_a), (0, mine, own_a)):
        (end,) = call(
            functools.partial(last_kernel, member, 0, width_y, members),
            f"last{member}",
            (core, obs_column, values, a) + tail,
            [half],
        )
        ends.append(end)
    other, own = ends
    back = lax.ppermute(other, "member", swap)
    return call(functools.partial(finish_kernel, width_y), "finish", (core, own, back), [(1, *anomalies.shape[1:])])[0]


def solution(mesh):
    in_specs = (
        P("member", None, None, "tile"),
        P(None, "tile"),
        P(),
        P(),
        P("member", None, "tile", None),
        P(),
        P(),
    )
    out_specs = P("member", None, "tile", None)
    return jax.shard_map(
        per_device, mesh=mesh, in_specs=in_specs, out_specs=out_specs, check_vma=False
    )
```

```python
import functools

import jax
import jax.numpy as jnp
from jax import lax
from jax.experimental import pallas as pl
from jax.experimental.pallas import tpu as pltpu
from jax.sharding import PartitionSpec as P

STEPS = 4
REACH = 8
VMEM = 24 << 20
PLANES = 4


MM = (((1,), (0,)), ((), ()))
TM = (((0,), (0,)), ((), ()))


def halves(x):
    high = x.astype(jnp.bfloat16)
    return high, (x - high.astype(jnp.float32)).astype(jnp.bfloat16)


def dot(a, b, dims=MM):
    part = lambda p, q: lax.dot_general(p, q, dims, preferred_element_type=jnp.float32)
    a_high, a_low = halves(a)
    b_high, b_low = halves(b)
    return part(a_high, b_high) + (part(a_high, b_low) + part(a_low, b_high))


def hot_rows(core, obs_row, sides, width_y):
    count = obs_row.shape[1]
    y = lax.broadcasted_iota(jnp.int32, (width_y, count), 0)
    hot = []
    for side in sides:
        x = jnp.where(core == 0, side, 3 - side)
        hot.append((obs_row == x * width_y + y).astype(jnp.bfloat16))
    return jnp.concatenate(hot, axis=0) if len(hot) > 1 else hot[0]


def placed(values, hot):
    return lax.dot_general(values, hot, (((0,), (1,)), ((), ())), preferred_element_type=jnp.float32)


def send_parts(lam, spread, physics, modes_ref, far_ref, near_ref, sums_ref, width_y):
    product = spread[0] * lam[0] + spread[1] * lam[1]
    local = dot(modes_ref[...], product)
    for copy in range(PLANES):
        sums_ref[copy] = local
    w = width_y
    matrix = physics[...]
    for m in range(2):
        moved = dot(matrix, lam[m], TM)
        far_ref[:, m * w : (m + 1) * w] = moved[:, :w]
        near_ref[:, m * w : (m + 1) * w] = moved[:, w:]


def prepare_kernel(width_y, core_ref, obs_ref, mine_hbm, anomalies_hbm, modes_ref, late_ref, sums_ref,
                   mine_ref, anomalies_ref, sems):
    copies = (
        pltpu.make_async_copy(mine_hbm.at[0, STEPS - 1], mine_ref, sems.at[0]),
        pltpu.make_async_copy(anomalies_hbm, anomalies_ref, sems.at[1]),
    )
    for copy in copies:
        copy.start()
    w = width_y
    order = (0, 1, 3, 2)
    count = obs_ref.shape[1]
    obs_row = obs_ref[STEPS - 1 : STEPS, :]
    y = lax.broadcasted_iota(jnp.int32, (w, count), 0)
    hot = jnp.concatenate([(obs_row == x * w + y).astype(jnp.bfloat16) for x in order], axis=0)
    copies[0].wait()
    values = mine_ref[...]
    late_ref[...] = values.astype(jnp.float32)
    lam = placed(values, hot)
    copies[1].wait()
    spread = jnp.concatenate([anomalies_ref[0, :, x, :].astype(jnp.float32) for x in order], axis=1)
    local = dot(modes_ref[...], spread * lam)
    for copy in range(PLANES):
        sums_ref[copy] = local


def column(row):
    n = row.shape[1]
    same = lax.broadcasted_iota(jnp.int32, (n, n), 0) == lax.broadcasted_iota(jnp.int32, (n, n), 1)
    return jnp.sum(jnp.where(same, row, 0.0), axis=1, keepdims=True)


def divide_kernel(width_y, core_ref, mine_ref, anomalies_ref, bands_ref, nu_ref, own_a_ref, rest_ref, bands_col_ref, nu_col_ref):
    bands_col_ref[...] = column(bands_ref[...].astype(jnp.float32)).astype(jnp.int32)
    nu_col_ref[...] = column(nu_ref[...])
    low = core_ref[0] == 0
    w = width_y
    rows = [anomalies_ref[0, :, x, :].astype(jnp.float32) for x in range(4)]
    state = rows[0].shape[0]
    count = mine_ref.shape[2]
    for i in range(2):
        own_a_ref[:, i * w : (i + 1) * w] = jnp.where(low, rows[i], rows[3 - i]).astype(jnp.bfloat16)
        rest_ref[:state, i * w : (i + 1) * w] = jnp.where(low, rows[3 - i], rows[i])
    for t in range(STEPS - 1):
        rest_ref[state + t * count : state + (t + 1) * count, :] = mine_ref[0, t].astype(jnp.float32)


def pass_on_kernel(core_ref, obs_ref, late_ref, other_ref, far_ref):
    count = late_ref.shape[0]
    far_ref[:count, :] = late_ref[...]
    far_ref[count : 2 * count, :] = other_ref[...]
    far_ref[2 * count :, :] = jnp.zeros((far_ref.shape[0] - 2 * count, far_ref.shape[1]), jnp.float32)
    far_ref[2 * count : 2 * count + 1, :count] = obs_ref[STEPS - 1 : STEPS, :].astype(jnp.float32)


def regroup_kernel(core_ref, sums_ref, out_ref):
    total = sums_ref[0] + sums_ref[1] + sums_ref[2] + sums_ref[3]
    half = total.shape[1] // 2
    for j in range(2 * PLANES):
        out_ref[j] = total[:, (j % 2) * half : (j % 2 + 1) * half]


def both_spreads(own_a_ref, other_a_ref):
    return own_a_ref[...].astype(jnp.float32), other_a_ref[...].astype(jnp.float32)


def smooth_of(total, bands, width_y, members):
    lane = lax.broadcasted_iota(jnp.int32, (total.shape[0], width_y), 1)
    halves = []
    for i in range(2):
        here = total[:, i * width_y : (i + 1) * width_y]
        out = here
        for off in range(1, REACH + 1):
            up = jnp.where(lane >= off, pltpu.roll(here, off, 1), 0.0)
            down = jnp.where(lane < width_y - off, pltpu.roll(here, width_y - off, 1), 0.0)
            out = out + jnp.where(bands >= off, up + down, 0.0)
        halves.append(out)
    whole = jnp.concatenate(halves, axis=1)
    return whole / ((members - 1) * (2 * bands + 1)).astype(jnp.float32)


def beside(row, width_y):
    lane = lax.broadcasted_iota(jnp.int32, row.shape, 1)
    up = jnp.where(lane >= 1, pltpu.roll(row, 1, 1), 0.0)
    down = jnp.where(lane < width_y - 1, pltpu.roll(row, width_y - 1, 1), 0.0)
    return up + down


def advance(moved, spread, force, smooth, modes_ref, nu_ref, width_y):
    lifted = dot(modes_ref[...], smooth, TM)
    nu = nu_ref[...]
    lam = []
    for m in range(2):
        far, near, out_near, out_far = moved[m]
        v_far = far + nu * (out_far + near + beside(far, width_y) - 4.0 * far)
        v_near = near + nu * (far + out_near + beside(near, width_y) - 4.0 * near)
        lam.append(jnp.concatenate([v_far, v_near], axis=1) + spread[m] * lifted + force[m])
    return lam


def forcings(step, core, obs_ref, mine_ref, other, width_y):
    hot = hot_rows(core, obs_ref[step : step + 1, :], (0, 1), width_y)
    return placed(mine_ref[0, step], hot), placed(other, hot)


def next_lam(step, width_y, members, core_ref, obs_ref, mine_ref, own_a_ref, other_a_ref, other_ref, modes_ref,
             bands_ref, nu_ref, sums_ref, far_sent, near_sent, far_ref, near_ref):
    w = width_y
    total = sums_ref[0] + sums_ref[1] + sums_ref[2] + sums_ref[3]
    smooth = smooth_of(total, bands_ref[...], w, members)
    spread = both_spreads(own_a_ref, other_a_ref)
    count = obs_ref.shape[1]
    other = other_ref[step * count : (step + 1) * count, :]
    force = forcings(step, core_ref[0], obs_ref, mine_ref, other, w)
    cut = lambda ref, m: ref[:, m * w : (m + 1) * w]
    moved = [
        (cut(far_sent, m), cut(near_sent, m), cut(near_ref, 1 - m), cut(far_ref, 1 - m)) for m in range(2)
    ]
    return advance(moved, spread, force, smooth, modes_ref, nu_ref, w), spread


def second_kernel(width_y, members, core_ref, obs_ref, mine_ref, own_a_ref, rest_ref, late_ref, beyond_ref, physics_ref,
                  modes_ref, bands_ref, nu_ref, sums_ref,
                  far_out, near_out, sums_out, other_a_ref, other_ref, first_matrix, matrix, sems):
    step = STEPS - 2
    copies = [pltpu.make_async_copy(physics_ref.at[step - i], (first_matrix, matrix)[i], sems.at[i]) for i in range(2)]
    for copy in copies:
        copy.start()
    core = core_ref[0]
    w = width_y
    state = own_a_ref.shape[0]
    count = obs_ref.shape[1]
    other_a_ref[...] = rest_ref[:state, :].astype(jnp.bfloat16)
    other_ref[...] = rest_ref[state:, :].astype(jnp.bfloat16)
    spread = both_spreads(own_a_ref, other_a_ref)
    hot = hot_rows(core, obs_ref[STEPS - 1 : STEPS, :], (0, 1, 2), w)
    far_hot = hot_rows(core, beyond_ref[2 * count : 2 * count + 1, :count].astype(jnp.int32), (3,), w)
    inside = (mine_ref[0, STEPS - 1], late_ref[...].astype(jnp.bfloat16))
    beyond = [beyond_ref[(1 - m) * count : (2 - m) * count, :].astype(jnp.bfloat16) for m in range(2)]
    copies[0].wait()
    turned = first_matrix[...]
    moved = []
    for m in range(2):
        lam = jnp.concatenate([placed(inside[m], hot), placed(beyond[m], far_hot)], axis=1)
        u = dot(turned, lam, TM)
        moved.append([u[:, i * w : (i + 1) * w] for i in range(4)])
    total = sums_ref[0]
    for j in range(1, 2 * PLANES):
        total = total + sums_ref[j]
    smooth = smooth_of(total, bands_ref[...], w, members)
    force = forcings(step, core, obs_ref, mine_ref, other_ref[step * count : (step + 1) * count, :], w)
    lam = advance(moved, spread, force, smooth, modes_ref, nu_ref, w)
    copies[1].wait()
    send_parts(lam, spread, matrix, modes_ref, far_out, near_out, sums_out, w)


def step_kernel(step, width_y, members, core_ref, obs_ref, mine_ref, own_a_ref, other_a_ref, other_ref, physics_ref,
                modes_ref, bands_ref, nu_ref, sums_ref, far_sent, near_sent, far_ref, near_ref,
                far_out, near_out, sums_out, matrix, sem):
    copy = pltpu.make_async_copy(physics_ref.at[step - 1], matrix, sem)
    copy.start()
    lam, spread = next_lam(step, width_y, members, core_ref, obs_ref, mine_ref, own_a_ref, other_a_ref, other_ref,
                           modes_ref, bands_ref, nu_ref, sums_ref, far_sent, near_sent, far_ref, near_ref)
    copy.wait()
    send_parts(lam, spread, matrix, modes_ref, far_out, near_out, sums_out, width_y)


def last_kernel(member, step, width_y, members, core_ref, obs_ref, values_ref, a_ref, modes_ref, bands_ref, nu_ref, sums_ref,
                far_sent, near_sent, far_ref, near_ref, out_ref):
    w = width_y
    total = sums_ref[0] + sums_ref[1] + sums_ref[2] + sums_ref[3]
    lifted = dot(modes_ref[...], smooth_of(total, bands_ref[...], w, members), TM)
    count = obs_ref.shape[1]
    values = values_ref[step * count : (step + 1) * count, :] if member else values_ref[0, step]
    force = placed(values, hot_rows(core_ref[0], obs_ref[step : step + 1, :], (0, 1), w))
    nu = nu_ref[...]
    cut = lambda ref, m: ref[:, m * w : (m + 1) * w]
    far, near, out_near, out_far = cut(far_sent, member), cut(near_sent, member), cut(near_ref, 1 - member), cut(far_ref, 1 - member)
    v_far = far + nu * (out_far + near + beside(far, w) - 4.0 * far)
    v_near = near + nu * (far + out_near + beside(near, w) - 4.0 * near)
    out_ref[...] = jnp.concatenate([v_far, v_near], axis=1) + a_ref[...].astype(jnp.float32) * lifted + force


def finish_kernel(width_y, core_ref, own_ref, back_ref, out_ref):
    low = core_ref[0] == 0
    w = width_y
    mine = (own_ref[:, :w], own_ref[:, w:])
    got = (back_ref[:, :w], back_ref[:, w:])
    when_low = (mine[0], mine[1], got[1], got[0])
    when_high = (got[0], got[1], mine[1], mine[0])
    for x in range(4):
        out_ref[0, :, x, :] = jnp.where(low, when_low[x], when_high[x])


def call(kernel, name, args, outs, types=(), hbm=(), scratch=(), flops=400_000_000):
    spaces = [pltpu.SMEM] + [pltpu.HBM if i in hbm else pltpu.VMEM for i in range(1, len(args))]
    types = tuple(types) or (jnp.float32,) * len(outs)
    return pl.pallas_call(
        kernel,
        in_specs=[pl.BlockSpec(memory_space=space) for space in spaces],
        out_specs=[pl.BlockSpec(memory_space=pltpu.VMEM)] * len(outs),
        out_shape=[jax.ShapeDtypeStruct(o, t) for o, t in zip(outs, types)],
        scratch_shapes=list(scratch),
        cost_estimate=pl.CostEstimate(flops=flops, bytes_accessed=2_000_000, transcendentals=0),
        compiler_params=pltpu.CompilerParams(vmem_limit_bytes=None if name == "prepare" else VMEM),
    )(*args)


def per_device(innovations, obs_column, physics, diffusion, anomalies, modes, bands):
    members = lax.axis_size("member")
    tiles = lax.axis_size("tile")
    _, state, _, width_y = anomalies.shape
    core = (lax.axis_index("member") & 1).astype(jnp.int32)[None]
    mine = jnp.swapaxes(innovations, 2, 3)
    count = mine.shape[2]
    modes_t = modes.T
    n_modes = modes.shape[1]

    swap = [(i, i ^ 1) for i in range(members)]
    far_pairs = []
    for m in range(members):
        for t in range(tiles):
            target = (t + 1) % tiles if m % 2 else (t - 1) % tiles
            far_pairs.append((m * tiles + t, (m ^ 1) * tiles + target))
    side = 2 * PLANES
    y_groups = [[side * y + j for y in range(PLANES)] for j in range(side)]
    z_groups = [[side * y + 2 * z + c for z in range(PLANES)] for y in range(PLANES) for c in range(2)]
    chip_groups = [[side * y + j for j in range(side)] for y in range(PLANES)]

    half = (state, 2 * width_y)
    matrix = pltpu.VMEM((state, state), jnp.float32)
    sums_shape = (PLANES, n_modes, 2 * width_y)
    late, sums = call(
        functools.partial(prepare_kernel, width_y),
        "prepare",
        (core, obs_column, mine, anomalies, modes_t),
        [(count, state), (PLANES, n_modes, 4 * width_y)],
        hbm=(2, 3),
        scratch=(
            pltpu.VMEM((count, state), mine.dtype),
            pltpu.VMEM(anomalies.shape, anomalies.dtype),
            pltpu.SemaphoreType.DMA((2,)),
        ),
    )
    sums = lax.all_to_all(sums, "member", 0, 0, tiled=True, axis_index_groups=y_groups)
    other_late = lax.ppermute(late, "member", swap)
    (beyond,) = call(pass_on_kernel, "pass_on", (core, obs_column, late, other_late), [(2 * count + 8, state)])
    beyond = lax.ppermute(beyond, ("member", "tile"), far_pairs)
    (sums,) = call(regroup_kernel, "regroup", (core, sums), [(side, n_modes, 2 * width_y)])
    sums = lax.all_to_all(sums, "member", 0, 0, tiled=True, axis_index_groups=chip_groups)
    mine_late, anomalies_late, _ = lax.optimization_barrier((mine, anomalies, other_late))
    own_a, rest, bands_col, nu_col = call(
        functools.partial(divide_kernel, width_y),
        "divide",
        (core, mine_late, anomalies_late, bands[None], diffusion[None]),
        [half, (state + (STEPS - 1) * count, 2 * width_y), (n_modes, 1), (state, 1)],
        types=(jnp.bfloat16, jnp.float32, jnp.int32, jnp.float32),
    )
    rest = lax.ppermute(rest, "member", swap)
    *sent, other_a, other_innov = call(
        functools.partial(second_kernel, width_y, members),
        "second",
        (core, obs_column, mine, own_a, rest, other_late, beyond, physics, modes_t, bands_col, nu_col, sums),
        [half, half, sums_shape, half, ((STEPS - 1) * count, state)],
        types=(jnp.float32,) * 3 + (jnp.bfloat16,) * 2,
        hbm=(7,),
        scratch=(matrix, matrix, pltpu.SemaphoreType.DMA((2,))),
    )
    known = (core, obs_column, mine, own_a, other_a, other_innov)
    for step in range(STEPS - 3, -1, -1):
        far_sent, near_sent, sums = sent
        far = lax.ppermute(far_sent, ("member", "tile"), far_pairs)
        sums = lax.all_to_all(sums, "member", 0, 0, tiled=True, axis_index_groups=y_groups)
        near = lax.ppermute(near_sent, "member", swap)
        sums = jnp.broadcast_to(sums.sum(axis=0)[None], sums_shape)
        sums = lax.all_to_all(sums, "member", 0, 0, tiled=True, axis_index_groups=z_groups)
        tail = (modes_t, bands_col, nu_col, sums, far_sent, near_sent, far, near)
        if step > 0:
            sent = call(
                functools.partial(step_kernel, step, width_y, members),
                f"step{step}",
                known + (physics,) + tail,
                [half, half, sums_shape],
                hbm=(6,),
                scratch=(matrix, pltpu.SemaphoreType.DMA),
            )
    ends = []
    for member, values, a in ((1, other_innov, other_a), (0, mine, own_a)):
        (end,) = call(
            functools.partial(last_kernel, member, 0, width_y, members),
            f"last{member}",
            (core, obs_column, values, a) + tail,
            [half],
        )
        ends.append(end)
    other, own = ends
    back = lax.ppermute(other, "member", swap)
    return call(functools.partial(finish_kernel, width_y), "finish", (core, own, back), [(1, *anomalies.shape[1:])])[0]


def solution(mesh):
    in_specs = (
        P("member", None, None, "tile"),
        P(None, "tile"),
        P(),
        P(),
        P("member", None, "tile", None),
        P(),
        P(),
    )
    out_specs = P("member", None, "tile", None)
    return jax.shard_map(
        per_device, mesh=mesh, in_specs=in_specs, out_specs=out_specs, check_vma=False
    )
```

```python
import functools

import jax
import jax.numpy as jnp
from jax import lax
from jax.experimental import pallas as pl
from jax.experimental.pallas import tpu as pltpu
from jax.sharding import PartitionSpec as P

STEPS = 4
REACH = 8
VMEM = 24 << 20
PLANES = 4


MM = (((1,), (0,)), ((), ()))
TM = (((0,), (0,)), ((), ()))


def halves(x):
    high = x.astype(jnp.bfloat16)
    return high, (x - high.astype(jnp.float32)).astype(jnp.bfloat16)


def dot(a, b, dims=MM):
    part = lambda p, q: lax.dot_general(p, q, dims, preferred_element_type=jnp.float32)
    a_high, a_low = halves(a)
    b_high, b_low = halves(b)
    return part(a_high, b_high) + (part(a_high, b_low) + part(a_low, b_high))


def hot_rows(core, obs_row, sides, width_y):
    count = obs_row.shape[1]
    y = lax.broadcasted_iota(jnp.int32, (width_y, count), 0)
    hot = []
    for side in sides:
        x = jnp.where(core == 0, side, 3 - side)
        hot.append((obs_row == x * width_y + y).astype(jnp.bfloat16))
    return jnp.concatenate(hot, axis=0) if len(hot) > 1 else hot[0]


def placed(values, hot):
    return lax.dot_general(values, hot, (((0,), (1,)), ((), ())), preferred_element_type=jnp.float32)


def send_parts(lam, spread, physics, modes_ref, far_ref, near_ref, sums_ref, width_y):
    product = spread[0] * lam[0] + spread[1] * lam[1]
    local = dot(modes_ref[...], product)
    for copy in range(PLANES):
        sums_ref[copy] = local
    w = width_y
    matrix = physics[...]
    for m in range(2):
        moved = dot(matrix, lam[m], TM)
        far_ref[:, m * w : (m + 1) * w] = moved[:, :w]
        near_ref[:, m * w : (m + 1) * w] = moved[:, w:]


def prepare_kernel(width_y, core_ref, obs_ref, mine_hbm, anomalies_hbm, modes_ref, late_ref, sums_ref,
                   mine_ref, anomalies_ref, sems):
    copies = (
        pltpu.make_async_copy(mine_hbm.at[0, STEPS - 1], mine_ref, sems.at[0]),
        pltpu.make_async_copy(anomalies_hbm, anomalies_ref, sems.at[1]),
    )
    for copy in copies:
        copy.start()
    w = width_y
    order = (0, 1, 3, 2)
    count = obs_ref.shape[1]
    obs_row = obs_ref[STEPS - 1 : STEPS, :]
    y = lax.broadcasted_iota(jnp.int32, (w, count), 0)
    hot = jnp.concatenate([(obs_row == x * w + y).astype(jnp.bfloat16) for x in order], axis=0)
    copies[0].wait()
    values = mine_ref[...]
    late_ref[...] = values.astype(jnp.float32)
    lam = placed(values, hot)
    copies[1].wait()
    spread = jnp.concatenate([anomalies_ref[0, :, x, :].astype(jnp.float32) for x in order], axis=1)
    local = dot(modes_ref[...], spread * lam)
    for copy in range(PLANES):
        sums_ref[copy] = local


def divide_kernel(width_y, core_ref, mine_ref, anomalies_ref, own_a_ref, rest_ref):
    low = core_ref[0] == 0
    w = width_y
    rows = [anomalies_ref[0, :, x, :].astype(jnp.float32) for x in range(4)]
    state = rows[0].shape[0]
    count = mine_ref.shape[2]
    for i in range(2):
        own_a_ref[:, i * w : (i + 1) * w] = jnp.where(low, rows[i], rows[3 - i]).astype(jnp.bfloat16)
        rest_ref[:state, i * w : (i + 1) * w] = jnp.where(low, rows[3 - i], rows[i])
    for t in range(STEPS - 1):
        rest_ref[state + t * count : state + (t + 1) * count, :] = mine_ref[0, t].astype(jnp.float32)


def pass_on_kernel(core_ref, obs_ref, late_ref, other_ref, far_ref):
    count = late_ref.shape[0]
    far_ref[:count, :] = late_ref[...]
    far_ref[count : 2 * count, :] = other_ref[...]
    far_ref[2 * count :, :] = jnp.zeros((far_ref.shape[0] - 2 * count, far_ref.shape[1]), jnp.float32)
    far_ref[2 * count : 2 * count + 1, :count] = obs_ref[STEPS - 1 : STEPS, :].astype(jnp.float32)


def regroup_kernel(core_ref, sums_ref, out_ref):
    total = sums_ref[0] + sums_ref[1] + sums_ref[2] + sums_ref[3]
    half = total.shape[1] // 2
    for j in range(2 * PLANES):
        out_ref[j] = total[:, (j % 2) * half : (j % 2 + 1) * half]


def both_spreads(own_a_ref, other_a_ref):
    return own_a_ref[...].astype(jnp.float32), other_a_ref[...].astype(jnp.float32)


def smooth_of(total, bands, width_y, members):
    lane = lax.broadcasted_iota(jnp.int32, (total.shape[0], width_y), 1)
    halves = []
    for i in range(2):
        here = total[:, i * width_y : (i + 1) * width_y]
        out = here
        for off in range(1, REACH + 1):
            up = jnp.where(lane >= off, pltpu.roll(here, off, 1), 0.0)
            down = jnp.where(lane < width_y - off, pltpu.roll(here, width_y - off, 1), 0.0)
            out = out + jnp.where(bands >= off, up + down, 0.0)
        halves.append(out)
    whole = jnp.concatenate(halves, axis=1)
    return whole / ((members - 1) * (2 * bands + 1)).astype(jnp.float32)


def beside(row, width_y):
    lane = lax.broadcasted_iota(jnp.int32, row.shape, 1)
    up = jnp.where(lane >= 1, pltpu.roll(row, 1, 1), 0.0)
    down = jnp.where(lane < width_y - 1, pltpu.roll(row, width_y - 1, 1), 0.0)
    return up + down


def advance(moved, spread, force, smooth, modes_ref, nu_ref, width_y):
    lifted = dot(modes_ref[...], smooth, TM)
    nu = nu_ref[...]
    lam = []
    for m in range(2):
        far, near, out_near, out_far = moved[m]
        v_far = far + nu * (out_far + near + beside(far, width_y) - 4.0 * far)
        v_near = near + nu * (far + out_near + beside(near, width_y) - 4.0 * near)
        lam.append(jnp.concatenate([v_far, v_near], axis=1) + spread[m] * lifted + force[m])
    return lam


def forcings(step, core, obs_ref, mine_ref, other, width_y):
    hot = hot_rows(core, obs_ref[step : step + 1, :], (0, 1), width_y)
    return placed(mine_ref[0, step], hot), placed(other, hot)


def next_lam(step, width_y, members, core_ref, obs_ref, mine_ref, own_a_ref, other_a_ref, other_ref, modes_ref,
             bands_ref, nu_ref, sums_ref, far_sent, near_sent, far_ref, near_ref):
    w = width_y
    total = sums_ref[0] + sums_ref[1] + sums_ref[2] + sums_ref[3]
    smooth = smooth_of(total, bands_ref[...], w, members)
    spread = both_spreads(own_a_ref, other_a_ref)
    count = obs_ref.shape[1]
    other = other_ref[step * count : (step + 1) * count, :]
    force = forcings(step, core_ref[0], obs_ref, mine_ref, other, w)
    cut = lambda ref, m: ref[:, m * w : (m + 1) * w]
    moved = [
        (cut(far_sent, m), cut(near_sent, m), cut(near_ref, 1 - m), cut(far_ref, 1 - m)) for m in range(2)
    ]
    return advance(moved, spread, force, smooth, modes_ref, nu_ref, w), spread


def second_kernel(width_y, members, core_ref, obs_ref, mine_ref, own_a_ref, rest_ref, late_ref, beyond_ref, first_matrix, matrix,
                  modes_ref, bands_ref, nu_ref, sums_ref,
                  far_out, near_out, sums_out, other_a_ref, other_ref):
    step = STEPS - 2
    core = core_ref[0]
    w = width_y
    state = own_a_ref.shape[0]
    count = obs_ref.shape[1]
    other_a_ref[...] = rest_ref[:state, :].astype(jnp.bfloat16)
    other_ref[...] = rest_ref[state:, :].astype(jnp.bfloat16)
    spread = both_spreads(own_a_ref, other_a_ref)
    hot = hot_rows(core, obs_ref[STEPS - 1 : STEPS, :], (0, 1, 2), w)
    far_hot = hot_rows(core, beyond_ref[2 * count : 2 * count + 1, :count].astype(jnp.int32), (3,), w)
    inside = (mine_ref[0, STEPS - 1], late_ref[...].astype(jnp.bfloat16))
    beyond = [beyond_ref[(1 - m) * count : (2 - m) * count, :].astype(jnp.bfloat16) for m in range(2)]
    turned = first_matrix[...]
    moved = []
    for m in range(2):
        lam = jnp.concatenate([placed(inside[m], hot), placed(beyond[m], far_hot)], axis=1)
        u = dot(turned, lam, TM)
        moved.append([u[:, i * w : (i + 1) * w] for i in range(4)])
    total = sums_ref[0]
    for j in range(1, 2 * PLANES):
        total = total + sums_ref[j]
    smooth = smooth_of(total, bands_ref[...], w, members)
    force = forcings(step, core, obs_ref, mine_ref, other_ref[step * count : (step + 1) * count, :], w)
    lam = advance(moved, spread, force, smooth, modes_ref, nu_ref, w)
    send_parts(lam, spread, matrix, modes_ref, far_out, near_out, sums_out, w)


def step_kernel(step, width_y, members, core_ref, obs_ref, mine_ref, own_a_ref, other_a_ref, other_ref, matrix,
                modes_ref, bands_ref, nu_ref, sums_ref, far_sent, near_sent, far_ref, near_ref,
                far_out, near_out, sums_out):
    lam, spread = next_lam(step, width_y, members, core_ref, obs_ref, mine_ref, own_a_ref, other_a_ref, other_ref,
                           modes_ref, bands_ref, nu_ref, sums_ref, far_sent, near_sent, far_ref, near_ref)
    send_parts(lam, spread, matrix, modes_ref, far_out, near_out, sums_out, width_y)


def last_kernel(member, step, width_y, members, core_ref, obs_ref, values_ref, a_ref, modes_ref, bands_ref, nu_ref, sums_ref,
                far_sent, near_sent, far_ref, near_ref, out_ref):
    w = width_y
    total = sums_ref[0] + sums_ref[1] + sums_ref[2] + sums_ref[3]
    lifted = dot(modes_ref[...], smooth_of(total, bands_ref[...], w, members), TM)
    count = obs_ref.shape[1]
    values = values_ref[step * count : (step + 1) * count, :] if member else values_ref[0, step]
    force = placed(values, hot_rows(core_ref[0], obs_ref[step : step + 1, :], (0, 1), w))
    nu = nu_ref[...]
    cut = lambda ref, m: ref[:, m * w : (m + 1) * w]
    far, near, out_near, out_far = cut(far_sent, member), cut(near_sent, member), cut(near_ref, 1 - member), cut(far_ref, 1 - member)
    v_far = far + nu * (out_far + near + beside(far, w) - 4.0 * far)
    v_near = near + nu * (far + out_near + beside(near, w) - 4.0 * near)
    out_ref[...] = jnp.concatenate([v_far, v_near], axis=1) + a_ref[...].astype(jnp.float32) * lifted + force


def finish_kernel(width_y, core_ref, own_ref, back_ref, out_ref):
    low = core_ref[0] == 0
    w = width_y
    mine = (own_ref[:, :w], own_ref[:, w:])
    got = (back_ref[:, :w], back_ref[:, w:])
    when_low = (mine[0], mine[1], got[1], got[0])
    when_high = (got[0], got[1], mine[1], mine[0])
    for x in range(4):
        out_ref[0, :, x, :] = jnp.where(low, when_low[x], when_high[x])


def call(kernel, name, args, outs, types=(), hbm=(), scratch=(), flops=400_000_000):
    spaces = [pltpu.SMEM] + [pltpu.HBM if i in hbm else pltpu.VMEM for i in range(1, len(args))]
    types = tuple(types) or (jnp.float32,) * len(outs)
    return pl.pallas_call(
        kernel,
        in_specs=[pl.BlockSpec(memory_space=space) for space in spaces],
        out_specs=[pl.BlockSpec(memory_space=pltpu.VMEM)] * len(outs),
        out_shape=[jax.ShapeDtypeStruct(o, t) for o, t in zip(outs, types)],
        scratch_shapes=list(scratch),
        cost_estimate=pl.CostEstimate(flops=flops, bytes_accessed=2_000_000, transcendentals=0),
        compiler_params=pltpu.CompilerParams(vmem_limit_bytes=None if name == "prepare" else VMEM),
    )(*args)


def per_device(innovations, obs_column, physics, diffusion, anomalies, modes, bands):
    members = lax.axis_size("member")
    tiles = lax.axis_size("tile")
    _, state, _, width_y = anomalies.shape
    core = (lax.axis_index("member") & 1).astype(jnp.int32)[None]
    mine = jnp.swapaxes(innovations, 2, 3)
    count = mine.shape[2]
    modes_t = modes.T
    n_modes = modes.shape[1]

    swap = [(i, i ^ 1) for i in range(members)]
    far_pairs = []
    for m in range(members):
        for t in range(tiles):
            target = (t + 1) % tiles if m % 2 else (t - 1) % tiles
            far_pairs.append((m * tiles + t, (m ^ 1) * tiles + target))
    side = 2 * PLANES
    y_groups = [[side * y + j for y in range(PLANES)] for j in range(side)]
    z_groups = [[side * y + 2 * z + c for z in range(PLANES)] for y in range(PLANES) for c in range(2)]
    chip_groups = [[side * y + j for j in range(side)] for y in range(PLANES)]

    half = (state, 2 * width_y)
    sums_shape = (PLANES, n_modes, 2 * width_y)
    bands_col = bands[:, None]
    nu_col = diffusion[:, None]
    late, sums = call(
        functools.partial(prepare_kernel, width_y),
        "prepare",
        (core, obs_column, mine, anomalies, modes_t),
        [(count, state), (PLANES, n_modes, 4 * width_y)],
        hbm=(2, 3),
        scratch=(
            pltpu.VMEM((count, state), mine.dtype),
            pltpu.VMEM(anomalies.shape, anomalies.dtype),
            pltpu.SemaphoreType.DMA((2,)),
        ),
    )
    sums = lax.all_to_all(sums, "member", 0, 0, tiled=True, axis_index_groups=y_groups)
    other_late = lax.ppermute(late, "member", swap)
    (beyond,) = call(pass_on_kernel, "pass_on", (core, obs_column, late, other_late), [(2 * count + 8, state)])
    beyond = lax.ppermute(beyond, ("member", "tile"), far_pairs)
    (sums,) = call(regroup_kernel, "regroup", (core, sums), [(side, n_modes, 2 * width_y)])
    sums = lax.all_to_all(sums, "member", 0, 0, tiled=True, axis_index_groups=chip_groups)
    mine_late, anomalies_late, _ = lax.optimization_barrier((mine, anomalies, other_late))
    own_a, rest = call(
        functools.partial(divide_kernel, width_y),
        "divide",
        (core, mine_late, anomalies_late),
        [half, (state + (STEPS - 1) * count, 2 * width_y)],
        types=(jnp.bfloat16, jnp.float32),
    )
    rest = lax.ppermute(rest, "member", swap)
    *sent, other_a, other_innov = call(
        functools.partial(second_kernel, width_y, members),
        "second",
        (core, obs_column, mine, own_a, rest, other_late, beyond, physics[STEPS - 2], physics[STEPS - 3], modes_t, bands_col, nu_col, sums),
        [half, half, sums_shape, half, ((STEPS - 1) * count, state)],
        types=(jnp.float32,) * 3 + (jnp.bfloat16,) * 2,
    )
    known = (core, obs_column, mine, own_a, other_a, other_innov)
    for step in range(STEPS - 3, -1, -1):
        far_sent, near_sent, sums = sent
        far = lax.ppermute(far_sent, ("member", "tile"), far_pairs)
        sums = lax.all_to_all(sums, "member", 0, 0, tiled=True, axis_index_groups=y_groups)
        near = lax.ppermute(near_sent, "member", swap)
        sums = jnp.broadcast_to(sums.sum(axis=0)[None], sums_shape)
        sums = lax.all_to_all(sums, "member", 0, 0, tiled=True, axis_index_groups=z_groups)
        tail = (modes_t, bands_col, nu_col, sums, far_sent, near_sent, far, near)
        if step > 0:
            sent = call(
                functools.partial(step_kernel, step, width_y, members),
                f"step{step}",
                known + (physics[step - 1],) + tail,
                [half, half, sums_shape],
            )
    ends = []
    for member, values, a in ((1, other_innov, other_a), (0, mine, own_a)):
        (end,) = call(
            functools.partial(last_kernel, member, 0, width_y, members),
            f"last{member}",
            (core, obs_column, values, a) + tail,
            [half],
        )
        ends.append(end)
    other, own = ends
    back = lax.ppermute(other, "member", swap)
    return call(functools.partial(finish_kernel, width_y), "finish", (core, own, back), [(1, *anomalies.shape[1:])])[0]


def solution(mesh):
    in_specs = (
        P("member", None, None, "tile"),
        P(None, "tile"),
        P(),
        P(),
        P("member", None, "tile", None),
        P(),
        P(),
    )
    out_specs = P("member", None, "tile", None)
    return jax.shard_map(
        per_device, mesh=mesh, in_specs=in_specs, out_specs=out_specs, check_vma=False
    )
```
